256 devices in a mesh: ctx: 128 (over z, y_hi, x, core), dp: 2 (over y_lo).
Axes of the slice: x: 4, y: 4 (y_hi: 2, y_lo: 2; y = y_hi * 2 + y_lo), z: 8, core: 2. Of those that a mesh axis runs over, the one named last changes fastest.
Arguments:
- queries: bfloat16 [32768, 1024], P(('dp', 'ctx')), parts along dimension 0, may hold values from -2.5 to 2.5
- keys: bfloat16 [32768, 128], P(('dp', 'ctx')), parts along dimension 0, may hold values from -2.5 to 2.5
- values: bfloat16 [32768, 128], P(('dp', 'ctx')), parts along dimension 0, may hold values from -6 to 6
- grad_out: bfloat16 [32768, 1024], P(('dp', 'ctx')), parts along dimension 0, may hold values from -6 to 6
- pair_order: int32 [256], P('dp'), parts along dimension 0, may hold values from 0 to 127, each once
- doc_lengths: int32 [32], P('dp'), parts along dimension 0, may hold values from 1 to 4096, 16384 in all
Outputs:
- attn_out: bfloat16 [32768, 1024], P(('dp', 'ctx')), parts along dimension 0
- query_grad: bfloat16 [32768, 1024], P(('dp', 'ctx')), parts along dimension 0
- key_grad: bfloat16 [32768, 128], P(('dp', 'ctx')), parts along dimension 0
- value_grad: bfloat16 [32768, 128], P(('dp', 'ctx')), parts along dimension 0
The draws below stay inside these ranges and needn't reach their ends.
There are 2 independent parts, one for each index of `dp`. The reference program is written for one: setup_inputs(seed, part) draws one part's arguments, and reference() takes and returns one part's arrays. A program takes and returns all parts, laid end to end along the dimension named above; each array names one. Nothing has to cross between parts.
Inputs may be any that keep to these rules, and one draw needn't show every extreme that they name: A permutation; the device of index d along ctx holds the sequence blocks pair_order[d] and 255 - pair_order[d], of 64 tokens each, in this order. `doc_lengths`: the documents lie end to end in sequence order; the lengths sum to 16384 and the longest has exactly 4096 tokens.
All inputs are finite; a program needn't handle non-finite values.
Results may differ from the reference program's by a relative error of at most 0.01.
Values may be sent and summed in bfloat16 or wider, within the bound.
No kernel may reach another device: no remote copies, remote signals or barrier semaphores. Data moves between devices by JAX's collectives and lax.ppermute only.
A program may use at most 128 MiB of HBM per device.

```python
import math
import jax
import jax.numpy as jnp
import numpy as np
from jax import lax

HEADS = 8
HDIM = 128
TOK_DEV = 128
DOCS = 16
HALF_DEV = 64
PAIRS = 128
SEQ = 16384


def draw_keys(key, part):
    first_key, second_key = jax.random.split(key, 2)
    row_scales = jnp.exp(jax.random.uniform(first_key, (SEQ, 1), jnp.float32, jnp.log(0.2), jnp.log(2.0)))
    base = jax.random.normal(second_key, (SEQ, HDIM), jnp.float32)
    return jnp.clip(base * row_scales, -2.5, 2.5).astype(jnp.bfloat16)


def block_scale(own_key, dims, cuts, low, top_value):
    def one(axis_at, parts):
        heights = jax.random.uniform(jax.random.fold_in(jax.random.fold_in(own_key, 6), axis_at), (parts,), jnp.float32, low / len(cuts), top_value / len(cuts))
        return jnp.repeat(jnp.exp(heights), dims[axis_at] // parts).reshape((-1,) + (1,) * (len(dims) - axis_at - 1))

    loudness = one(*cuts[0])
    for cut in cuts[1:]:
        loudness = loudness * one(*cut)
    return loudness


def length_profile(number_of, total, reach, skew):
    portions = [(1 << 20) // math.isqrt(standing ** skew) + 1 for standing in range(2, number_of + 1)]
    rest, holding = total - reach - (number_of - 1), [1] * (number_of - 1)
    while rest > 0:
        candidates = [i for i in range(number_of - 1) if holding[i] < reach]
        whole, remaining = sum([portions[i] for i in candidates]), rest
        for i in candidates:
            extra = min(reach - holding[i], max(1, remaining * portions[i] // whole), rest)
            holding[i] = holding[i] + extra
            rest = rest - extra
    return np.array([reach] + holding)


def uneven(stream_key, number_of, total, limit, skew):
    if number_of == 2:
        one = jax.random.randint(stream_key, (), max(1, total - limit), min(limit, total - 1) + 1)
        return jnp.stack([one, total - one])
    tallies = jnp.asarray(length_profile(number_of, total, limit, skew), jnp.int32)
    couples = (number_of - 1) // 2
    source_of, taker = tallies[1:1 + 2 * couples:2], tallies[2:2 + 2 * couples:2]
    room = jnp.minimum(source_of - 1, limit - taker)
    moved = jax.random.randint(jax.random.fold_in(stream_key, 1), (couples,), 0, 1 << 20) % (room + 1)
    tallies = tallies.at[1:1 + 2 * couples:2].set(source_of - moved).at[2:2 + 2 * couples:2].set(taker + moved)
    return tallies[jax.random.permutation(jax.random.fold_in(stream_key, 2), number_of)]


def centred(rng, extent, spread, most, pieces=(), kind=jnp.bfloat16):
    level = block_scale(rng, extent, pieces, -0.22, 0.18) if pieces else 1.0
    values = jax.random.normal(rng, extent, jnp.float32) * spread * level
    return jnp.minimum(jnp.maximum(values, -most), most).astype(kind)


def setup_inputs(seed: int = 0, part: int = 0) -> dict:
    streams_of = jax.random.split(jax.random.key(seed), 7)
    part_splits = jax.random.split(jax.random.fold_in(streams_of[6], part), 7)
    queries = centred(part_splits[0], (SEQ, HEADS * HDIM), 1.0, 2.5, ((0, 128),))
    keys = draw_keys(jax.random.fold_in(jax.random.fold_in(streams_of[6], part), 71), part)
    values = centred(part_splits[2], (SEQ, HDIM), 1.0, 6.0, ((0, 128),))
    grad_out = centred(part_splits[3], (SEQ, HEADS * HDIM), 1.0, 6.0, ((0, 128),))
    pair_order = jax.random.permutation(part_splits[4], PAIRS).astype(jnp.int32)
    doc_lengths = uneven(part_splits[5], DOCS, SEQ, SEQ // 4, 2).astype(jnp.int32)
    return dict(queries=queries, keys=keys, values=values, grad_out=grad_out, pair_order=pair_order, doc_lengths=doc_lengths)


def token_labels(pair_order, doc_lengths):
    row_ids = jnp.arange(SEQ, dtype=jnp.int32)
    shard_ids = row_ids // TOK_DEV
    inside = row_ids % TOK_DEV
    paired = pair_order[shard_ids].astype(jnp.int32)
    seq_block = jnp.where(inside < HALF_DEV, paired, 2 * PAIRS - 1 - paired)
    position = (seq_block * HALF_DEV + inside % HALF_DEV).astype(jnp.int32)
    doc_ends = jnp.cumsum(doc_lengths).astype(jnp.int32)
    document = jnp.sum((doc_ends[None, :] <= position[:, None]).astype(jnp.int32), axis=1)
    return position, document


def reference(queries, keys, values, grad_out, pair_order, doc_lengths):
    position, document = token_labels(pair_order, doc_lengths)
    score_scale = HDIM ** -0.5
    highest = lax.Precision.HIGHEST
    keys_f32 = keys.astype(jnp.float32)
    values_f32 = values.astype(jnp.float32)
    query_block = min(SEQ, 256)
    block_count = SEQ // query_block
    query_parts = queries.reshape(block_count, query_block, HEADS, HDIM)
    grad_parts = grad_out.reshape(block_count, query_block, HEADS, HDIM)
    pos_parts = position.reshape(block_count, query_block)
    doc_parts = document.reshape(block_count, query_block)

    def one_block(carried, sliced):
        key_acc, value_acc = carried
        query_rows, grad_rows, query_pos, query_doc = sliced
        query_f32 = query_rows.astype(jnp.float32)
        grad_f32 = grad_rows.astype(jnp.float32)
        allowed = (query_doc[:, None] == document[None, :]) & (position[None, :] <= query_pos[:, None])
        scores = jnp.einsum("thd,kd->thk", query_f32, keys_f32, precision=highest) * score_scale
        exp_scores = jnp.where(allowed[:, None, :], jnp.exp(scores), jnp.float32(0.0))
        totals = jnp.sum(exp_scores, axis=2)
        weight_b = lax.optimization_barrier(exp_scores.astype(jnp.bfloat16)).astype(jnp.float32)
        attn_out = (jnp.einsum("thk,kd->thd", weight_b, values_f32, precision=highest) / totals[:, :, None]).astype(jnp.bfloat16)
        log_totals = jnp.log(totals)
        row_dots = jnp.sum(grad_f32 * attn_out.astype(jnp.float32), axis=2)
        prob_f32 = jnp.where(allowed[:, None, :], jnp.exp(scores - log_totals[:, :, None]), jnp.float32(0.0))
        prob_b = lax.optimization_barrier(prob_f32.astype(jnp.bfloat16)).astype(jnp.float32)
        grad_prob = jnp.einsum("thd,kd->thk", grad_f32, values_f32, precision=highest)
        grad_score = lax.optimization_barrier((prob_f32 * (grad_prob - row_dots[:, :, None])).astype(jnp.bfloat16)).astype(jnp.float32)
        query_grad = (score_scale * jnp.einsum("thk,kd->thd", grad_score, keys_f32, precision=highest)).astype(jnp.bfloat16)
        key_acc = key_acc + jnp.einsum("thk,thd->kd", grad_score, query_f32, precision=highest)
        value_acc = value_acc + jnp.einsum("thk,thd->kd", prob_b, grad_f32, precision=highest)
        return (key_acc, value_acc), (attn_out, query_grad)

    start_sums = (jnp.zeros((SEQ, HDIM), jnp.float32), jnp.zeros((SEQ, HDIM), jnp.float32))
    final_sums, stacked = lax.scan(one_block, start_sums, (query_parts, grad_parts, pos_parts, doc_parts))
    attn_out = stacked[0].reshape(SEQ, HEADS * HDIM)
    query_grad = stacked[1].reshape(SEQ, HEADS * HDIM)
    key_grad = (score_scale * final_sums[0]).astype(jnp.bfloat16)
    value_grad = final_sums[1].astype(jnp.bfloat16)
    return (attn_out, query_grad, key_grad, value_grad)
```

```python
import functools

import jax
import jax.numpy as jnp
from jax import lax
from jax.experimental import pallas as pl
from jax.experimental.pallas import tpu as pltpu
from jax.sharding import Mesh
from jax.sharding import PartitionSpec as P

DIMS = (8, 2, 4, 2)
AXES = ("z", "y", "x", "core")
DP_CTX = ("dp",) + AXES

LOG2E = 1.4426950408889634


def attention_kernel(
    half,
    heads,
    hdim,
    docs,
    blocks,
    per_tile,
    table,
    q_ref,
    g_ref,
    *refs,
):
    pieces, refs = refs[: len(PLACES)], refs[len(PLACES) :]
    out_ref, dq_ref, dk_own, dk_other, dv_own, dv_other = refs[:6]
    k_all, v_all, dk_acc, dv_acc, weights, out_t, dq_t, totals, sems = refs[6:]
    copies = []
    for piece, (name, source, target, count) in zip(pieces, PLACES, strict=True):
        whole = k_all if name == "k" else v_all
        copies.append(
            pltpu.make_async_copy(
                piece.at[pl.ds(source, count), :],
                whole.at[pl.ds(target, count), :],
                sems.at[len(copies)],
            )
        )
    for copy in copies:
        copy.start()
    rows = half * heads
    tile = per_tile * half
    scale = hdim ** (-0.5)
    seq = half * blocks

    def clear(i, carry):
        at = pl.ds(pl.multiple_of(i * 256, 256), 256)
        dk_acc[at, :] = jnp.zeros((256, hdim), jnp.float32)
        dv_acc[at, :] = jnp.zeros((256, hdim), jnp.float32)
        return carry

    lax.fori_loop(0, seq // 256, clear, 0)
    for copy in copies:
        copy.wait()

    def doc_start(position):
        start = jnp.zeros_like(position)
        for d in range(docs):
            end = table[blocks + d]
            start = jnp.where(end <= position, jnp.maximum(start, end), start)
        return start

    def one_block(b, carry):
        own = pl.ds(pl.multiple_of(b * half, half), half)
        block = table[blocks + docs + b]
        first = block * half
        head = [slice(h * hdim, (h + 1) * hdim) for h in range(heads)]
        q_rows = jnp.concatenate([q_ref[own, s] for s in head], axis=0)
        g_rows = jnp.concatenate([g_ref[own, s] for s in head], axis=0)
        q_t = q_rows.T
        g_t = g_rows.T
        lane = lax.broadcasted_iota(jnp.int32, (1, rows), 1)
        position = first + lax.rem(lane, half)
        start = doc_start(position)
        low = jnp.int32(0)
        for d in range(docs):
            end = table[blocks + d]
            low = jnp.where(end <= first, jnp.maximum(low, end), low)
        low_block = lax.div(low, half)
        steps = lax.div(block - low_block + per_tile, per_tile)

        def places(i):
            found = []
            for u in range(per_tile):
                s = jnp.minimum(low_block + i * per_tile + u, block)
                found.append(pl.ds(pl.multiple_of(table[s], half), half))
            return found

        out_t[...] = jnp.zeros_like(out_t)
        dq_t[...] = jnp.zeros_like(dq_t)
        totals[...] = jnp.zeros_like(totals)

        def forward(i, carry):
            at = places(i)
            k_tile = jnp.concatenate([k_all[p, :] for p in at], axis=0)
            v_tile = jnp.concatenate([v_all[p, :] for p in at], axis=0)
            s_t = jnp.dot(k_tile, q_t, preferred_element_type=jnp.float32)
            key = (low_block + i * per_tile) * half + lax.broadcasted_iota(jnp.int32, (tile, 1), 0)
            allowed = (key >= start) & (key <= position)
            e_t = jnp.where(allowed, jnp.exp2(s_t * (scale * LOG2E)), 0.0)
            totals[...] += jnp.sum(e_t.reshape(tile // 8, 8, rows), axis=0)
            w_t = e_t.astype(jnp.bfloat16)
            weights[pl.ds(pl.multiple_of(i * tile, tile), tile), :] = w_t
            out_t[...] += lax.dot_general(
                v_tile, w_t, (((0,), (0,)), ((), ())), preferred_element_type=jnp.float32
            )
            return carry

        lax.fori_loop(0, steps, forward, 0)
        total = jnp.sum(totals[...], axis=0, keepdims=True)
        o_t = (out_t[...] / total).astype(jnp.bfloat16).astype(jnp.float32)
        o_rows = o_t.T.astype(jnp.bfloat16)
        for h, s in enumerate(head):
            out_ref[own, s] = o_rows[h * half : (h + 1) * half, :]
        row_dot = jnp.sum(g_t.astype(jnp.float32) * o_t, axis=0, keepdims=True)
        inverse = 1.0 / total

        def backward(i, carry):
            at = places(i)
            k_tile = jnp.concatenate([k_all[p, :] for p in at], axis=0)
            v_tile = jnp.concatenate([v_all[p, :] for p in at], axis=0)
            dp_t = jnp.dot(v_tile, g_t, preferred_element_type=jnp.float32)
            w_t = weights[pl.ds(pl.multiple_of(i * tile, tile), tile), :].astype(jnp.float32)
            p_t = w_t * inverse
            ds_t = (p_t * (dp_t - row_dot)).astype(jnp.bfloat16)
            p_b = p_t.astype(jnp.bfloat16)
            dq_t[...] += lax.dot_general(
                k_tile, ds_t, (((0,), (0,)), ((), ())), preferred_element_type=jnp.float32
            )
            dk = jnp.dot(ds_t, q_rows, preferred_element_type=jnp.float32)
            dv = jnp.dot(p_b, g_rows, preferred_element_type=jnp.float32)
            for u, p in enumerate(at):
                dk_acc[p, :] += dk[u * half : (u + 1) * half, :]
                dv_acc[p, :] += dv[u * half : (u + 1) * half, :]
            return carry

        lax.fori_loop(0, steps, backward, 0)
        dq_rows = (dq_t[...] * scale).T.astype(jnp.bfloat16)
        for h, s in enumerate(head):
            dq_ref[own, s] = dq_rows[h * half : (h + 1) * half, :]
        return carry

    lax.fori_loop(0, 2, one_block, 0)

    def finish(i, carry):
        at = pl.ds(pl.multiple_of(i * 256, 256), 256)
        far = pl.ds(pl.multiple_of(seq // 2 + i * 256, 256), 256)
        dk_own[at, :] = (dk_acc[at, :] * scale).astype(jnp.bfloat16)
        dk_other[at, :] = (dk_acc[far, :] * scale).astype(jnp.bfloat16)
        dv_own[at, :] = dv_acc[at, :].astype(jnp.bfloat16)
        dv_other[at, :] = dv_acc[far, :].astype(jnp.bfloat16)
        return carry

    lax.fori_loop(0, seq // 512, finish, 0)


def attention(table, queries, grad_out, pieces, half, docs, blocks):
    tokens, width = queries.shape
    hdim = pieces[0].shape[1]
    heads = width // hdim
    seq = half * blocks
    rows = half * heads
    per_tile = 4
    most = -(-(4096 // half + 1) // per_tile) * per_tile * half
    vmem = pl.BlockSpec(memory_space=pltpu.VMEM)
    wide = jax.ShapeDtypeStruct((tokens, width), jnp.bfloat16)
    term = jax.ShapeDtypeStruct((seq // 2, hdim), jnp.bfloat16)
    pairs = seq * 1600 * heads
    return pl.pallas_call(
        functools.partial(attention_kernel, half, heads, hdim, docs, blocks, per_tile),
        out_shape=(wide, wide, term, term, term, term),
        in_specs=[pl.BlockSpec(memory_space=pltpu.SMEM), vmem, vmem]
        + [pl.BlockSpec(memory_space=pl.ANY)] * len(pieces),
        out_specs=(vmem,) * 6,
        scratch_shapes=[
            pltpu.VMEM((seq, hdim), jnp.bfloat16),
            pltpu.VMEM((seq, hdim), jnp.bfloat16),
            pltpu.VMEM((seq, hdim), jnp.float32),
            pltpu.VMEM((seq, hdim), jnp.float32),
            pltpu.VMEM((most, rows), jnp.bfloat16),
            pltpu.VMEM((hdim, rows), jnp.float32),
            pltpu.VMEM((hdim, rows), jnp.float32),
            pltpu.VMEM((8, rows), jnp.float32),
            pltpu.SemaphoreType.DMA((len(pieces),)),
        ],
        compiler_params=pltpu.CompilerParams(vmem_limit_bytes=48 * 1024 * 1024),
        cost_estimate=pl.CostEstimate(
            flops=14 * hdim * pairs, bytes_accessed=4 * seq * hdim * 4, transcendentals=pairs
        ),
        name="attention",
    )(table, queries, grad_out, *pieces)


def place_table(pair_order, doc_lengths, tokens, half):
    devices = pair_order.shape[0]
    blocks = 2 * devices
    device = jnp.arange(devices, dtype=jnp.int32)
    slot = lax.rem(device % 2 + lax.axis_index("core"), 2)
    slot = slot * 4 + lax.rem(device // 2 % 4 - lax.axis_index("x") + 4, 4)
    slot = slot * 2 + lax.rem(device // 8 % 2 + lax.axis_index("y"), 2)
    slot = slot * 8 + device // 16
    block = jnp.arange(blocks, dtype=jnp.int32)
    pair = jnp.minimum(block, blocks - 1 - block)
    row = jnp.sum(
        jnp.where(pair_order[None, :] == pair[:, None], (slot * tokens)[None, :], 0), axis=1
    )
    row = row + jnp.where(block >= devices, half, 0)
    docs = jnp.arange(doc_lengths.shape[0], dtype=jnp.int32)
    ends = jnp.sum(jnp.where(docs[None, :] <= docs[:, None], doc_lengths[None, :], 0), axis=1)
    mine = jnp.sum(jnp.where(device == lax.axis_index(AXES), pair_order, 0))
    own = jnp.stack([mine, blocks - 1 - mine])
    return jnp.concatenate([row, ends, own]).astype(jnp.int32)


def from_x(a, step):
    return lax.ppermute(a, "x", [((i + step) % 4, i) for i in range(4)])


def swap(a, axis):
    return lax.ppermute(a, axis, [(0, 1), (1, 0)])


HALF_PLACES = (
    ("k", 0, 0, 2048),
    ("k", 0, 2048, 2048),
    ("k", 0, 6144, 2048),
    ("k", 0, 4096, 1024),
    ("k", 0, 5120, 1024),
    ("v", 0, 0, 1024),
    ("v", 0, 2048, 1024),
    ("v", 1024, 6144, 1024),
    ("v", 0, 4096, 1024),
    ("v", 0, 1024, 1024),
    ("v", 0, 3072, 1024),
    ("v", 1024, 7168, 1024),
    ("v", 0, 5120, 1024),
)
PLACES = HALF_PLACES + tuple((n, s, t + 8192, c) for n, s, t, c in HALF_PLACES)


def gathered(keys, values):
    hdim = keys.shape[1]
    kv = jnp.concatenate([keys, values], axis=1)
    column = lax.all_to_all(jnp.tile(kv, (8, 1)), "z", 0, 0, tiled=True)
    k, v = column[:, :hdim], column[:, hdim:]
    n = k.shape[0]
    k = jnp.concatenate([k, swap(k, "y")], axis=0)
    k_right, k_left = from_x(k, 1), from_x(k, 3)
    v_right, v_left = from_x(v, 1), from_x(v, 3)
    v_far = swap(v, "y")
    k_mid_0, k_mid_1 = from_x(k_right[:n], 1), from_x(k_left[n:], 3)
    v_mid_0, v_mid_1 = from_x(v_right[: n // 2], 1), from_x(v_left[n // 2 :], 3)
    v_side = jnp.concatenate([v_right, v_left], axis=0)
    v_side_far = swap(v_side, "y")
    v_mid = jnp.concatenate([v_mid_0, v_mid_1], axis=0)
    v_mid_far = swap(v_mid, "y")
    arrays = (k, k_right, k_left, k_mid_0, k_mid_1)
    arrays += (v, v_side, v_mid, v_far, v_side_far, v_mid_far)
    both = (arrays, tuple(swap(a, "core") for a in arrays))
    pieces = []
    for k0, k1, k2, k3, k4, v0, v1, v2, v3, v4, v5 in both:
        pieces += [k0, k1, k2, k3, k4, v0, v1, v1, v2, v3, v4, v4, v5]
    return pieces


def added(*terms):
    return sum(t.astype(jnp.float32) for t in terms).astype(jnp.bfloat16)


def reduced_x(near, right, mid, left):
    n = mid.shape[0] // 2
    to_right, to_left = from_x(mid[:n], 3), from_x(mid[n:], 1)
    right = jnp.concatenate([added(right[:n], to_right), right[n:]], axis=0)
    left = jnp.concatenate([left[:n], added(left[n:], to_left)], axis=0)
    return added(near, from_x(right, 3), from_x(left, 1))


def scattered(dk_own, dk_other, dv_own, dv_other, tokens):
    dv_in, dk_in = swap(dv_other, "core"), swap(dk_other, "core")
    n = 8 * tokens

    def dv(place):
        return added(dv_own[place * n : (place + 1) * n], dv_in[place * n : (place + 1) * n])

    mid_in = swap(dv(5), "y")
    side_in = swap(jnp.concatenate([dv(3), dv(7)], axis=0), "y")
    near_in = swap(dv(1), "y")
    dk = [added(dk_own[i : i + 2 * n], dk_in[i : i + 2 * n]) for i in range(0, 8 * n, 2 * n)]
    dk = reduced_x(*dk)
    dk = added(dk[:n], swap(dk[n:], "y"))
    dv = reduced_x(
        added(dv(0), near_in), added(dv(2), side_in[:n]), added(dv(4), mid_in), added(dv(6), side_in[n:])
    )
    column = lax.all_to_all(jnp.concatenate([dk, dv], axis=1), "z", 0, 0, tiled=True)
    column = column.reshape(8, tokens, -1).astype(jnp.float32)
    return jnp.sum(column, axis=0).astype(jnp.bfloat16)


def shards(queries, keys, values, grad_out, pair_order, doc_lengths):
    tokens, hdim = keys.shape
    half = tokens // 2
    table = place_table(pair_order, doc_lengths, tokens, half)
    pieces = gathered(keys, values)
    out, query_grad, *terms = attention(
        table, queries, grad_out, pieces, half, doc_lengths.shape[0], 2 * pair_order.shape[0]
    )
    grads = scattered(*terms, tokens)
    return out, query_grad, grads[:, :hdim], grads[:, hdim:]


def solution(mesh):
    torus = Mesh(mesh.devices.reshape(*DIMS, mesh.shape["dp"]), AXES + ("dp",))
    rows = P(DP_CTX, None)
    return jax.shard_map(
        shards,
        mesh=torus,
        in_specs=(rows, rows, rows, rows, P("dp"), P("dp")),
        out_specs=(rows, rows, rows, rows),
        check_vma=False,
    )
```

```python
import functools

import jax
import jax.numpy as jnp
from jax import lax
from jax.experimental import pallas as pl
from jax.experimental.pallas import tpu as pltpu
from jax.sharding import Mesh
from jax.sharding import PartitionSpec as P

DIMS = (8, 2, 4, 2)
AXES = ("z", "y", "x", "core")
DP_CTX = ("dp",) + AXES
GROUP = 4
LOG2E = 1.4426950408889634
FAR = 1 << 20


class Sizes:
    def __init__(self, tokens, width, hdim, devices, docs):
        self.half = tokens // 2
        self.tokens = tokens
        self.width = width
        self.hdim = hdim
        self.heads = width // hdim
        self.rows = self.half * self.heads
        self.docs = docs
        self.local = 2 * devices // GROUP
        self.keys = self.local * self.half
        self.queries = 2 * GROUP
        self.per_tile = 4
        self.tile = self.per_tile * self.half
        self.scale = hdim ** (-0.5)
        self.at_address = 0
        self.at_block = self.local
        self.at_ends = 2 * self.local
        self.at_own = self.at_ends + docs
        self.at_low = self.at_own + self.queries
        self.at_high = self.at_low + self.queries


def loaded(sizes, q_pieces, g_pieces, kv_pieces, q_all, g_all, kv_all, sems):
    copies = []
    for pieces, whole in ((q_pieces, q_all), (g_pieces, g_all), (kv_pieces, kv_all)):
        for i, piece in enumerate(pieces):
            count = piece.shape[0]
            target = whole.at[pl.ds(i * count, count), :]
            copies.append(pltpu.make_async_copy(piece, target, sems.at[len(copies)]))
    for copy in copies:
        copy.start()
    return copies


class Block:
    def __init__(self, sizes, table, b, q_all, g_all):
        self.sizes, self.table = sizes, table
        half, hdim = sizes.half, sizes.hdim
        self.own = pl.ds(pl.multiple_of(b * half, half), half)
        self.head = [slice(h * hdim, (h + 1) * hdim) for h in range(sizes.heads)]
        self.q_rows = jnp.concatenate([q_all[self.own, s] for s in self.head], axis=0)
        self.g_rows = jnp.concatenate([g_all[self.own, s] for s in self.head], axis=0)
        self.q_t = self.q_rows.T
        self.g_t = self.g_rows.T
        lane = lax.broadcasted_iota(jnp.int32, (1, sizes.rows), 1)
        self.position = table[sizes.at_own + b] * half + lax.rem(lane, half)
        start = jnp.zeros_like(self.position)
        for d in range(sizes.docs):
            end = table[sizes.at_ends + d]
            start = jnp.where(end <= self.position, jnp.maximum(start, end), start)
        self.start = start
        self.low = table[sizes.at_low + b]
        self.high = table[sizes.at_high + b]
        self.steps = lax.div(self.high - self.low + sizes.per_tile - 1, sizes.per_tile)

    def tile(self, i, kv_all):
        sizes, half, hdim = self.sizes, self.sizes.half, self.sizes.hdim
        places, keys = [], []
        inside = lax.broadcasted_iota(jnp.int32, (half, 1), 0)
        for u in range(sizes.per_tile):
            rank = self.low + i * sizes.per_tile + u
            held = jnp.minimum(rank, self.high - 1)
            place = pl.multiple_of(self.table[sizes.at_address + held], half)
            places.append(pl.ds(place, half))
            first = jnp.where(rank < self.high, self.table[sizes.at_block + held] * half, FAR)
            keys.append(first + inside)
        key = jnp.concatenate(keys, axis=0)
        k_tile = jnp.concatenate([kv_all[p, 0:hdim] for p in places], axis=0)
        v_tile = jnp.concatenate([kv_all[p, hdim : 2 * hdim] for p in places], axis=0)
        s_t = jnp.dot(k_tile, self.q_t, preferred_element_type=jnp.float32)
        allowed = (key >= self.start) & (key <= self.position)
        e_t = jnp.where(allowed, jnp.exp2(s_t * (sizes.scale * LOG2E)), 0.0)
        return places, k_tile, v_tile, e_t

    def put(self, ref, value_t):
        rows = value_t.T.astype(ref.dtype)
        for h, s in enumerate(self.head):
            ref[self.own, s] = rows[h * self.sizes.half : (h + 1) * self.sizes.half, :]


def transposed_product(tile, weights):
    dims = (((0,), (0,)), ((), ()))
    return lax.dot_general(tile, weights, dims, preferred_element_type=jnp.float32)


def forward_kernel(sizes, table, *refs):
    kv_count = len(refs) - 2 * GROUP - 8
    q_pieces, g_pieces = refs[:GROUP], refs[GROUP : 2 * GROUP]
    kv_pieces = refs[2 * GROUP : 2 * GROUP + kv_count]
    out_ref, stats_ref, q_all, g_all, kv_all, out_t, totals, sems = refs[-8:]
    copies = loaded(sizes, q_pieces, g_pieces, kv_pieces, q_all, g_all, kv_all, sems)
    for copy in copies:
        copy.wait()

    def one_block(b, carry):
        block = Block(sizes, table, b, q_all, g_all)
        out_t[...] = jnp.zeros_like(out_t)
        totals[...] = jnp.zeros_like(totals)

        def step(i, inner):
            _, _, v_tile, e_t = block.tile(i, kv_all)
            totals[...] += jnp.sum(e_t.reshape(sizes.tile // 8, 8, sizes.rows), axis=0)
            out_t[...] += transposed_product(v_tile, e_t.astype(jnp.bfloat16))
            return inner

        lax.fori_loop(0, block.steps, step, 0)
        o_t = out_t[...]
        total = jnp.sum(totals[...], axis=0, keepdims=True)
        row_dot = jnp.sum(block.g_t.astype(jnp.float32) * o_t, axis=0, keepdims=True)
        stats_ref[b] = jnp.concatenate([total, row_dot], axis=0)
        block.put(out_ref, o_t)
        return carry

    lax.fori_loop(0, sizes.queries, one_block, 0)


def backward_kernel(sizes, table, *refs):
    kv_count = len(refs) - 2 * GROUP - 10
    q_pieces, g_pieces = refs[:GROUP], refs[GROUP : 2 * GROUP]
    kv_pieces = refs[2 * GROUP : 2 * GROUP + kv_count]
    stats_ref, dq_ref, own_ref, other_ref, q_all, g_all, kv_all, acc, dq_t, sems = refs[-10:]
    hdim, half = sizes.hdim, sizes.half
    copies = loaded(sizes, q_pieces, g_pieces, kv_pieces, q_all, g_all, kv_all, sems)

    def clear(i, carry):
        at = pl.ds(pl.multiple_of(i * 256, 256), 256)
        acc[at, :] = jnp.zeros((256, 2 * hdim), jnp.float32)
        return carry

    lax.fori_loop(0, sizes.keys // 256, clear, 0)
    for copy in copies:
        copy.wait()

    def one_block(b, carry):
        block = Block(sizes, table, b, q_all, g_all)
        dq_t[...] = jnp.zeros_like(dq_t)
        stats = stats_ref[b]
        inverse = 1.0 / stats[0:1, :]
        row_dot = stats[1:2, :] * inverse

        def step(i, inner):
            places, k_tile, v_tile, e_t = block.tile(i, kv_all)
            dp_t = jnp.dot(v_tile, block.g_t, preferred_element_type=jnp.float32)
            p_t = e_t * inverse
            ds_t = (p_t * (dp_t - row_dot)).astype(jnp.bfloat16)
            p_b = p_t.astype(jnp.bfloat16)
            dq_t[...] += transposed_product(k_tile, ds_t)
            dk = jnp.dot(ds_t, block.q_rows, preferred_element_type=jnp.float32)
            dv = jnp.dot(p_b, block.g_rows, preferred_element_type=jnp.float32)
            for u, p in enumerate(places):
                acc[p, 0:hdim] += dk[u * half : (u + 1) * half, :]
                acc[p, hdim : 2 * hdim] += dv[u * half : (u + 1) * half, :]
            return inner

        lax.fori_loop(0, block.steps, step, 0)
        block.put(dq_ref, dq_t[...] * sizes.scale)
        return carry

    lax.fori_loop(0, sizes.queries, one_block, 0)

    def finish(i, carry):
        at = pl.ds(pl.multiple_of(i * 256, 256), 256)
        far = pl.ds(pl.multiple_of(sizes.keys // 2 + i * 256, 256), 256)
        own_ref[at, 0:hdim] = (acc[at, 0:hdim] * sizes.scale).astype(jnp.bfloat16)
        own_ref[at, hdim : 2 * hdim] = acc[at, hdim : 2 * hdim].astype(jnp.bfloat16)
        other_ref[at, 0:hdim] = (acc[far, 0:hdim] * sizes.scale).astype(jnp.bfloat16)
        other_ref[at, hdim : 2 * hdim] = acc[far, hdim : 2 * hdim].astype(jnp.bfloat16)
        return carry

    lax.fori_loop(0, sizes.keys // 512, finish, 0)


VMEM_SPEC = pl.BlockSpec(memory_space=pltpu.VMEM)
SMEM_SPEC = pl.BlockSpec(memory_space=pltpu.SMEM)
ANY_SPEC = pl.BlockSpec(memory_space=pl.ANY)


def held_arrays(sizes):
    wide = pltpu.VMEM((GROUP * sizes.tokens, sizes.width), jnp.bfloat16)
    return [wide, wide, pltpu.VMEM((sizes.keys, 2 * sizes.hdim), jnp.bfloat16)]


def cost(sizes, products):
    pairs = sizes.keys * sizes.queries * sizes.rows // 4
    return pl.CostEstimate(
        flops=2 * products * sizes.hdim * pairs, bytes_accessed=6 << 20, transcendentals=pairs
    )


def forward(sizes, table, q_pieces, g_pieces, kv_pieces):
    pieces = (*q_pieces, *g_pieces, *kv_pieces)
    wide = jax.ShapeDtypeStruct((GROUP * sizes.tokens, sizes.width), jnp.bfloat16)
    return pl.pallas_call(
        functools.partial(forward_kernel, sizes),
        out_shape=(wide, jax.ShapeDtypeStruct((sizes.queries, 2, sizes.rows), jnp.float32)),
        in_specs=[SMEM_SPEC] + [ANY_SPEC] * len(pieces),
        out_specs=(VMEM_SPEC, VMEM_SPEC),
        scratch_shapes=held_arrays(sizes)
        + [
            pltpu.VMEM((sizes.hdim, sizes.rows), jnp.float32),
            pltpu.VMEM((8, sizes.rows), jnp.float32),
            pltpu.SemaphoreType.DMA((len(pieces),)),
        ],
        compiler_params=pltpu.CompilerParams(vmem_limit_bytes=24 * 1024 * 1024),
        cost_estimate=cost(sizes, 2),
        name="forward",
    )(table, *pieces)


def backward(sizes, table, q_pieces, g_pieces, kv_pieces, stats):
    pieces = (*q_pieces, *g_pieces, *kv_pieces)
    wide = jax.ShapeDtypeStruct((GROUP * sizes.tokens, sizes.width), jnp.bfloat16)
    term = jax.ShapeDtypeStruct((sizes.keys // 2, 2 * sizes.hdim), jnp.bfloat16)
    return pl.pallas_call(
        functools.partial(backward_kernel, sizes),
        out_shape=(wide, term, term),
        in_specs=[SMEM_SPEC] + [ANY_SPEC] * len(pieces) + [VMEM_SPEC],
        out_specs=(VMEM_SPEC, VMEM_SPEC, VMEM_SPEC),
        scratch_shapes=held_arrays(sizes)
        + [
            pltpu.VMEM((sizes.keys, 2 * sizes.hdim), jnp.float32),
            pltpu.VMEM((sizes.hdim, sizes.rows), jnp.float32),
            pltpu.SemaphoreType.DMA((len(pieces),)),
        ],
        compiler_params=pltpu.CompilerParams(vmem_limit_bytes=32 * 1024 * 1024),
        cost_estimate=cost(sizes, 6),
        name="backward",
    )(table, *pieces, stats)


def index_table(sizes, pair_order, doc_lengths, z, y, x, core):
    devices = pair_order.shape[0]
    device = jnp.arange(devices, dtype=jnp.int32)
    slot = lax.rem(device % 2 + core, 2) * 2 + lax.rem(device // 8 % 2 + y, 2)
    row = (slot * 8 + device // 16) * sizes.tokens
    mirrored = 2 * devices - 1 - pair_order
    block = jnp.concatenate([pair_order, mirrored])
    row = jnp.concatenate([row, row + sizes.half])
    local = device // 2 % 4 == x
    local = jnp.concatenate([local, local])
    rank = jnp.sum((local[None, :] & (block[None, :] < block[:, None])).astype(jnp.int32), axis=1)
    place = jnp.arange(sizes.local, dtype=jnp.int32)
    chosen = local[None, :] & (rank[None, :] == place[:, None])
    address = jnp.sum(jnp.where(chosen, row[None, :], 0), axis=1)
    held = jnp.sum(jnp.where(chosen, block[None, :], 0), axis=1)
    docs = jnp.arange(sizes.docs, dtype=jnp.int32)
    ends = jnp.sum(jnp.where(docs[None, :] <= docs[:, None], doc_lengths[None, :], 0), axis=1)
    query = jnp.arange(sizes.queries, dtype=jnp.int32)
    owner = z * 16 + y * 8 + lax.rem(x + query // 2, 4) * 2 + core
    own = jnp.sum(jnp.where(owner[:, None] == device[None, :], pair_order[None, :], 0), axis=1)
    own = jnp.where(query % 2 == 0, own, 2 * devices - 1 - own)
    first = own * sizes.half
    start = jnp.max(jnp.where(ends[None, :] <= first[:, None], ends[None, :], 0), axis=1)
    low = jnp.sum((held[None, :] < (start // sizes.half)[:, None]).astype(jnp.int32), axis=1)
    high = jnp.sum((held[None, :] <= own[:, None]).astype(jnp.int32), axis=1)
    return jnp.concatenate([address, held, ends, own, low, high]).astype(jnp.int32)


def from_x(a, step):
    return lax.ppermute(a, "x", [((i + step) % 4, i) for i in range(4)])


def swap(a, axis):
    return lax.ppermute(a, axis, [(0, 1), (1, 0)])


def added(*terms):
    return sum(t.astype(jnp.float32) for t in terms).astype(jnp.bfloat16)


def gathered_x(queries, grad_out):
    q_right, q_left = from_x(queries, 1), from_x(queries, 3)
    g_right, g_left = from_x(grad_out, 1), from_x(grad_out, 3)
    q_mid, g_mid = from_x(q_right, 1), from_x(g_left, 3)
    return (queries, q_right, q_mid, q_left), (grad_out, g_right, g_mid, g_left)


def gathered_keys(keys, values):
    kv = jnp.concatenate([keys, values], axis=1)
    near = lax.all_to_all(jnp.tile(kv, (8, 1)), "z", 0, 0, tiled=True)
    far = swap(near, "y")
    return near, far, swap(near, "core"), swap(far, "core")


def scattered_keys(own, other, tokens):
    n = 8 * tokens
    other = swap(other, "core")
    far = swap(added(own[n:], other[n:]), "y")
    column = added(own[:n], other[:n], far)
    column = lax.all_to_all(column, "z", 0, 0, tiled=True)
    column = column.reshape(8, tokens, -1).astype(jnp.float32)
    return jnp.sum(column, axis=0).astype(jnp.bfloat16)


def summed_x(parts, tokens):
    part = [parts[i * tokens : (i + 1) * tokens] for i in range(GROUP)]
    return [part[0]] + [from_x(part[(4 - step) % 4], step) for step in (1, 3, 2)]


def shared_stats(stats):
    total = stats
    for step in (1, 3, 2):
        total = total + jnp.roll(from_x(stats, step), 2 * step, axis=0)
    return total


def shards(queries, keys, values, grad_out, pair_order, doc_lengths):
    tokens, hdim = keys.shape
    width = queries.shape[1]
    sizes = Sizes(tokens, width, hdim, pair_order.shape[0], doc_lengths.shape[0])
    spot = [lax.axis_index(a) for a in AXES]
    table = index_table(sizes, pair_order, doc_lengths, *spot)
    q_pieces, g_pieces = gathered_x(queries, grad_out)
    kv_pieces = gathered_keys(keys, values)
    out_parts, stats = forward(sizes, table, q_pieces, g_pieces, kv_pieces)
    stats = shared_stats(stats)
    out_parts = summed_x(out_parts, tokens)
    dq_parts, own, other = backward(sizes, table, q_pieces, g_pieces, kv_pieces, stats)
    total = stats[:2, 0, :].reshape(2, sizes.heads, sizes.half)
    total = jnp.swapaxes(total, 1, 2).reshape(tokens, sizes.heads, 1)
    out = sum(p.astype(jnp.float32) for p in out_parts).reshape(tokens, sizes.heads, hdim)
    out = (out / total).astype(jnp.bfloat16).reshape(tokens, width)
    query_grad = added(*summed_x(dq_parts, tokens))
    grads = scattered_keys(own, other, tokens)
    return out, query_grad, grads[:, :hdim], grads[:, hdim:]


def solution(mesh):
    torus = Mesh(mesh.devices.reshape(*DIMS, mesh.shape["dp"]), AXES + ("dp",))
    rows = P(DP_CTX, None)
    return jax.shard_map(
        shards,
        mesh=torus,
        in_specs=(rows, rows, rows, rows, P("dp"), P("dp")),
        out_specs=(rows, rows, rows, rows),
        check_vma=False,
    )
```

```python
import functools

import jax
import jax.numpy as jnp
from jax import lax
from jax.experimental import pallas as pl
from jax.experimental.pallas import tpu as pltpu
from jax.sharding import Mesh
from jax.sharding import PartitionSpec as P

DIMS = (8, 2, 4, 2)
AXES = ("z", "y", "x", "core")
DP_CTX = ("dp",) + AXES
GROUP = 4
LOG2E = 1.4426950408889634
FAR = 1 << 20


class Sizes:
    def __init__(self, tokens, width, hdim, devices, docs):
        self.half = tokens // 2
        self.tokens = tokens
        self.width = width
        self.hdim = hdim
        self.heads = width // hdim
        self.rows = self.half * self.heads
        self.docs = docs
        self.local = 2 * devices // GROUP
        self.keys = self.local * self.half
        self.queries = 2 * GROUP
        self.per_tile = 4
        self.tile = self.per_tile * self.half
        self.scale = hdim ** (-0.5)
        self.at_key = 0
        self.at_value = self.local
        self.at_block = 2 * self.local
        self.at_ends = 3 * self.local
        self.at_own = self.at_ends + docs
        self.at_low = self.at_own + self.queries
        self.at_high = self.at_low + self.queries


def loaded(sizes, pieces, q_all, g_all, k_all, v_all, sems):
    moves = []
    tokens = sizes.tokens
    for i, piece in enumerate(pieces[:GROUP]):
        at = pl.ds(i * tokens, tokens)
        moves.append((piece.at[pl.ds(0, tokens), :], q_all.at[at, :]))
        moves.append((piece.at[pl.ds(tokens, tokens), :], g_all.at[at, :]))
    for part, whole in ((pieces[GROUP:-2], k_all), (pieces[-2:], v_all)):
        for i, piece in enumerate(part):
            count = piece.shape[0]
            moves.append((piece, whole.at[pl.ds(i * count, count), :]))
    copies = [pltpu.make_async_copy(*move, sems.at[i]) for i, move in enumerate(moves)]
    for copy in copies:
        copy.start()
    return copies


class Block:
    def __init__(self, sizes, table, b, q_all, g_all):
        self.sizes, self.table = sizes, table
        half, hdim = sizes.half, sizes.hdim
        self.own = pl.ds(pl.multiple_of(b * half, half), half)
        self.head = [slice(h * hdim, (h + 1) * hdim) for h in range(sizes.heads)]
        self.q_rows = jnp.concatenate([q_all[self.own, s] for s in self.head], axis=0)
        self.g_rows = jnp.concatenate([g_all[self.own, s] for s in self.head], axis=0)
        self.q_t = self.q_rows.T
        self.g_t = self.g_rows.T
        lane = lax.broadcasted_iota(jnp.int32, (1, sizes.rows), 1)
        self.position = table[sizes.at_own + b] * half + lax.rem(lane, half)
        start = jnp.zeros_like(self.position)
        for d in range(sizes.docs):
            end = table[sizes.at_ends + d]
            start = jnp.where(end <= self.position, jnp.maximum(start, end), start)
        self.start = start
        self.low = table[sizes.at_low + b]
        self.high = table[sizes.at_high + b]
        self.steps = lax.div(self.high - self.low + sizes.per_tile - 1, sizes.per_tile)

    def tile(self, i, k_all, v_all):
        sizes, half = self.sizes, self.sizes.half
        k_at, v_at, keys = [], [], []
        inside = lax.broadcasted_iota(jnp.int32, (half, 1), 0)
        for u in range(sizes.per_tile):
            rank = self.low + i * sizes.per_tile + u
            held = jnp.minimum(rank, self.high - 1)
            k_at.append(pl.ds(pl.multiple_of(self.table[sizes.at_key + held], half), half))
            v_at.append(pl.ds(pl.multiple_of(self.table[sizes.at_value + held], half), half))
            first = jnp.where(rank < self.high, self.table[sizes.at_block + held] * half, FAR)
            keys.append(first + inside)
        key = jnp.concatenate(keys, axis=0)
        k_tile = jnp.concatenate([k_all[p, :] for p in k_at], axis=0)
        v_tile = jnp.concatenate([v_all[p, :] for p in v_at], axis=0)
        s_t = jnp.dot(k_tile, self.q_t, preferred_element_type=jnp.float32)
        allowed = (key >= self.start) & (key <= self.position)
        e_t = jnp.where(allowed, jnp.exp2(s_t * (sizes.scale * LOG2E)), 0.0)
        return k_at, v_at, k_tile, v_tile, e_t

    def put(self, ref, value_t):
        rows = value_t.T.astype(ref.dtype)
        for h, s in enumerate(self.head):
            ref[self.own, s] = rows[h * self.sizes.half : (h + 1) * self.sizes.half, :]


def transposed_product(tile, weights):
    dims = (((0,), (0,)), ((), ()))
    return lax.dot_general(tile, weights, dims, preferred_element_type=jnp.float32)


def forward_kernel(sizes, table, *refs):
    pieces, refs = refs[:-9], refs[-9:]
    out_ref, stats_ref, q_all, g_all, k_all, v_all, out_t, totals, sems = refs
    copies = loaded(sizes, pieces, q_all, g_all, k_all, v_all, sems)
    for copy in copies:
        copy.wait()

    def one_block(b, carry):
        block = Block(sizes, table, b, q_all, g_all)
        out_t[...] = jnp.zeros_like(out_t)
        totals[...] = jnp.zeros_like(totals)

        def step(i, inner):
            _, _, _, v_tile, e_t = block.tile(i, k_all, v_all)
            totals[...] += jnp.sum(e_t.reshape(sizes.tile // 8, 8, sizes.rows), axis=0)
            out_t[...] += transposed_product(v_tile, e_t.astype(jnp.bfloat16))
            return inner

        lax.fori_loop(0, block.steps, step, 0)
        o_t = out_t[...]
        total = jnp.sum(totals[...], axis=0, keepdims=True)
        row_dot = jnp.sum(block.g_t.astype(jnp.float32) * o_t, axis=0, keepdims=True)
        stats_ref[b] = jnp.concatenate([total, row_dot], axis=0)
        block.put(out_ref, o_t)
        return carry

    lax.fori_loop(0, sizes.queries, one_block, 0)


def backward_kernel(sizes, table, *refs):
    pieces, refs = refs[:-14], refs[-14:]
    stats_ref, dq_ref, dk_own, dk_other, dv_own, dv_other = refs[:6]
    q_all, g_all, k_all, v_all, dk_acc, dv_acc, dq_t, sems = refs[6:]
    half = sizes.half
    copies = loaded(sizes, pieces, q_all, g_all, k_all, v_all, sems)

    def clear(i, carry):
        at = pl.ds(pl.multiple_of(i * 256, 256), 256)
        dk_acc[at, :] = jnp.zeros((256, sizes.hdim), jnp.float32)
        dv_acc[at, :] = jnp.zeros((256, sizes.hdim), jnp.float32)
        return carry

    lax.fori_loop(0, sizes.keys // 256, clear, 0)
    for copy in copies:
        copy.wait()

    def one_block(b, carry):
        block = Block(sizes, table, b, q_all, g_all)
        dq_t[...] = jnp.zeros_like(dq_t)
        stats = stats_ref[b]
        inverse = 1.0 / stats[0:1, :]
        row_dot = stats[1:2, :] * inverse

        def step(i, inner):
            k_at, v_at, k_tile, v_tile, e_t = block.tile(i, k_all, v_all)
            dp_t = jnp.dot(v_tile, block.g_t, preferred_element_type=jnp.float32)
            p_t = e_t * inverse
            ds_t = (p_t * (dp_t - row_dot)).astype(jnp.bfloat16)
            p_b = p_t.astype(jnp.bfloat16)
            dq_t[...] += transposed_product(k_tile, ds_t)
            dk = jnp.dot(ds_t, block.q_rows, preferred_element_type=jnp.float32)
            dv = jnp.dot(p_b, block.g_rows, preferred_element_type=jnp.float32)
            for u in range(sizes.per_tile):
                dk_acc[k_at[u], :] += dk[u * half : (u + 1) * half, :]
                dv_acc[v_at[u], :] += dv[u * half : (u + 1) * half, :]
            return inner

        lax.fori_loop(0, block.steps, step, 0)
        block.put(dq_ref, dq_t[...] * sizes.scale)
        return carry

    lax.fori_loop(0, sizes.queries, one_block, 0)

    def finish(i, carry):
        at = pl.ds(pl.multiple_of(i * 256, 256), 256)
        far = pl.ds(pl.multiple_of(sizes.keys // 2 + i * 256, 256), 256)
        dk_own[at, :] = (dk_acc[at, :] * sizes.scale).astype(jnp.bfloat16)
        dk_other[at, :] = (dk_acc[far, :] * sizes.scale).astype(jnp.bfloat16)
        dv_own[at, :] = dv_acc[at, :].astype(jnp.bfloat16)
        dv_other[at, :] = dv_acc[far, :].astype(jnp.bfloat16)
        return carry

    lax.fori_loop(0, sizes.keys // 512, finish, 0)


VMEM_SPEC = pl.BlockSpec(memory_space=pltpu.VMEM)
SMEM_SPEC = pl.BlockSpec(memory_space=pltpu.SMEM)
HBM_SPEC = pl.BlockSpec(memory_space=pltpu.HBM)


def held_arrays(sizes):
    wide = pltpu.VMEM((GROUP * sizes.tokens, sizes.width), jnp.bfloat16)
    narrow = pltpu.VMEM((sizes.keys, sizes.hdim), jnp.bfloat16)
    return [wide, wide, narrow, narrow]


def cost(sizes, products):
    pairs = sizes.keys * sizes.queries * sizes.rows // 4
    return pl.CostEstimate(
        flops=2 * products * sizes.hdim * pairs, bytes_accessed=6 << 20, transcendentals=pairs
    )


def forward(sizes, table, pieces):
    wide = jax.ShapeDtypeStruct((GROUP * sizes.tokens, sizes.width), jnp.bfloat16)
    return pl.pallas_call(
        functools.partial(forward_kernel, sizes),
        out_shape=(wide, jax.ShapeDtypeStruct((sizes.queries, 2, sizes.rows), jnp.float32)),
        in_specs=[SMEM_SPEC] + [HBM_SPEC] * len(pieces),
        out_specs=(VMEM_SPEC, VMEM_SPEC),
        scratch_shapes=held_arrays(sizes)
        + [
            pltpu.VMEM((sizes.hdim, sizes.rows), jnp.float32),
            pltpu.VMEM((8, sizes.rows), jnp.float32),
            pltpu.SemaphoreType.DMA((len(pieces) + GROUP,)),
        ],
        compiler_params=pltpu.CompilerParams(vmem_limit_bytes=24 * 1024 * 1024),
        cost_estimate=cost(sizes, 2),
        name="forward",
    )(table, *pieces)


def backward(sizes, table, pieces, stats):
    wide = jax.ShapeDtypeStruct((GROUP * sizes.tokens, sizes.width), jnp.bfloat16)
    term = jax.ShapeDtypeStruct((sizes.keys // 2, sizes.hdim), jnp.bfloat16)
    return pl.pallas_call(
        functools.partial(backward_kernel, sizes),
        out_shape=(wide, term, term, term, term),
        in_specs=[SMEM_SPEC] + [HBM_SPEC] * len(pieces) + [VMEM_SPEC],
        out_specs=(VMEM_SPEC,) * 5,
        scratch_shapes=held_arrays(sizes)
        + [
            pltpu.VMEM((sizes.keys, sizes.hdim), jnp.float32),
            pltpu.VMEM((sizes.keys, sizes.hdim), jnp.float32),
            pltpu.VMEM((sizes.hdim, sizes.rows), jnp.float32),
            pltpu.SemaphoreType.DMA((len(pieces) + GROUP,)),
        ],
        compiler_params=pltpu.CompilerParams(vmem_limit_bytes=32 * 1024 * 1024),
        cost_estimate=cost(sizes, 6),
        name="backward",
    )(table, *pieces, stats)


def index_table(sizes, pair_order, doc_lengths, z, y, x, core):
    devices = pair_order.shape[0]
    device = jnp.arange(devices, dtype=jnp.int32)
    far_core, far_y = lax.rem(device % 2 + core, 2), lax.rem(device // 8 % 2 + y, 2)
    k_row = (far_core * 16 + far_y * 8 + device // 16) * sizes.tokens
    v_row = (far_core * 16 + device // 16 * 2 + far_y) * sizes.tokens
    mirrored = 2 * devices - 1 - pair_order
    block = jnp.concatenate([pair_order, mirrored])
    k_row = jnp.concatenate([k_row, k_row + sizes.half])
    v_row = jnp.concatenate([v_row, v_row + sizes.half])
    local = device // 2 % 4 == x
    local = jnp.concatenate([local, local])
    rank = jnp.sum((local[None, :] & (block[None, :] < block[:, None])).astype(jnp.int32), axis=1)
    place = jnp.arange(sizes.local, dtype=jnp.int32)
    chosen = local[None, :] & (rank[None, :] == place[:, None])
    k_at = jnp.sum(jnp.where(chosen, k_row[None, :], 0), axis=1)
    v_at = jnp.sum(jnp.where(chosen, v_row[None, :], 0), axis=1)
    held = jnp.sum(jnp.where(chosen, block[None, :], 0), axis=1)
    docs = jnp.arange(sizes.docs, dtype=jnp.int32)
    ends = jnp.sum(jnp.where(docs[None, :] <= docs[:, None], doc_lengths[None, :], 0), axis=1)
    query = jnp.arange(sizes.queries, dtype=jnp.int32)
    owner = z * 16 + y * 8 + lax.rem(x + query // 2, 4) * 2 + core
    own = jnp.sum(jnp.where(owner[:, None] == device[None, :], pair_order[None, :], 0), axis=1)
    own = jnp.where(query % 2 == 0, own, 2 * devices - 1 - own)
    first = own * sizes.half
    start = jnp.max(jnp.where(ends[None, :] <= first[:, None], ends[None, :], 0), axis=1)
    low = jnp.sum((held[None, :] < (start // sizes.half)[:, None]).astype(jnp.int32), axis=1)
    high = jnp.sum((held[None, :] <= own[:, None]).astype(jnp.int32), axis=1)
    return jnp.concatenate([k_at, v_at, held, ends, own, low, high]).astype(jnp.int32)


def from_x(a, step):
    return lax.ppermute(a, "x", [((i + step) % 4, i) for i in range(4)])


def swap(a, axis):
    return lax.ppermute(a, axis, [(0, 1), (1, 0)])


def added(*terms):
    return sum(t.astype(jnp.float32) for t in terms).astype(jnp.bfloat16)


def over_z(a):
    return lax.all_to_all(a, "z", 0, 0, tiled=True)


def gathered_x(queries, grad_out):
    both = jnp.concatenate([queries, grad_out], axis=0)
    pieces = [both]
    for step in (1, 2, 3):
        pieces.append(from_x(both, step))
    return pieces


def gathered_keys(keys, values):
    values = jnp.concatenate([values, swap(values, "y")], axis=0)
    k_near = over_z(jnp.tile(keys, (8, 1)))
    v = over_z(jnp.tile(values, (8, 1)))
    k_far = swap(k_near, "y")
    return [k_near, k_far, swap(k_near, "core"), swap(k_far, "core"), v, swap(v, "core")]


def scattered_keys(own, other, tokens):
    n = 8 * tokens
    other = swap(other, "core")
    far = swap(added(own[n:], other[n:]), "y")
    column = over_z(added(own[:n], other[:n], far))
    column = column.reshape(8, tokens, -1).astype(jnp.float32)
    return jnp.sum(column, axis=0).astype(jnp.bfloat16)


def scattered_values(own, other, tokens):
    other = swap(other, "core")
    column = over_z(added(own, other))
    column = column.reshape(8, 2 * tokens, -1).astype(jnp.float32)
    column = jnp.sum(column, axis=0)
    far = swap(column[tokens:].astype(jnp.bfloat16), "y")
    return added(column[:tokens], far)


def summed_x(parts, tokens):
    part = [parts[i * tokens : (i + 1) * tokens] for i in range(GROUP)]
    received = [part[0]]
    for step in (1, 2, 3):
        received.append(from_x(part[(4 - step) % 4], step))
    return received


def shared_stats(stats):
    total = stats
    for step in (1, 2, 3):
        arrived = from_x(stats, step)
        total = total + jnp.roll(arrived, 2 * step, axis=0)
    return total


def grads_of(queries, keys, values, grad_out, pair_order, doc_lengths):
    tokens, hdim = keys.shape
    width = queries.shape[1]
    sizes = Sizes(tokens, width, hdim, pair_order.shape[0], doc_lengths.shape[0])
    spot = [lax.axis_index(a) for a in AXES]
    table = index_table(sizes, pair_order, doc_lengths, *spot)
    pieces = gathered_x(queries, grad_out) + gathered_keys(keys, values)
    out_parts, stats = forward(sizes, table, pieces)
    stats = shared_stats(stats)
    out_parts = summed_x(out_parts, tokens)
    dq_parts, *terms = backward(sizes, table, pieces, stats)
    total = stats[:2, 0, :].reshape(2, sizes.heads, sizes.half)
    total = jnp.swapaxes(total, 1, 2).reshape(tokens, sizes.heads, 1)
    out = sum(p.astype(jnp.float32) for p in out_parts).reshape(tokens, sizes.heads, hdim)
    out = (out / total).astype(jnp.bfloat16).reshape(tokens, width)
    query_grad = added(*summed_x(dq_parts, tokens))
    key_grad = scattered_keys(*terms[:2], tokens)
    value_grad = scattered_values(*terms[2:], tokens)
    return out, query_grad, key_grad, value_grad


def solution(mesh):
    torus = Mesh(mesh.devices.reshape(*DIMS, mesh.shape["dp"]), AXES + ("dp",))
    rows = P(DP_CTX, None)
    return jax.shard_map(
        grads_of,
        mesh=torus,
        in_specs=(rows, rows, rows, rows, P("dp"), P("dp")),
        out_specs=(rows, rows, rows, rows),
        check_vma=False,
    )
```

```python
import functools

import jax
import jax.numpy as jnp
from jax import lax
from jax.experimental import pallas as pl
from jax.experimental.pallas import tpu as pltpu
from jax.sharding import Mesh
from jax.sharding import PartitionSpec as P

DIMS = (8, 2, 4, 2)
AXES = ("z", "y", "x", "core")
DP_CTX = ("dp",) + AXES
GROUP = 4
LOG2E = 1.4426950408889634
FAR = 1 << 20


class Sizes:
    def __init__(self, tokens, width, hdim, devices, docs):
        self.half = tokens // 2
        self.tokens = tokens
        self.width = width
        self.hdim = hdim
        self.heads = width // hdim
        self.rows = self.half * self.heads
        self.docs = docs
        self.local = 2 * devices // GROUP
        self.keys = self.local * self.half
        self.queries = 2 * GROUP
        self.per_tile = 4
        self.tile = self.per_tile * self.half
        self.scale = hdim ** (-0.5)
        self.at_key = 0
        self.at_value = self.local
        self.at_block = 2 * self.local
        self.at_ends = 3 * self.local
        self.at_own = self.at_ends + docs
        self.at_low = self.at_own + self.queries
        self.at_high = self.at_low + self.queries


def loaded(sizes, pieces, q_all, g_all, k_all, v_all, sems):
    moves = []
    tokens = sizes.tokens
    for i, piece in enumerate(pieces[:GROUP]):
        at = pl.ds(i * tokens, tokens)
        moves.append((piece.at[pl.ds(0, tokens), :], q_all.at[at, :]))
        moves.append((piece.at[pl.ds(tokens, tokens), :], g_all.at[at, :]))
    for part, whole in ((pieces[GROUP:-2], k_all), (pieces[-2:], v_all)):
        for i, piece in enumerate(part):
            count = piece.shape[0]
            moves.append((piece, whole.at[pl.ds(i * count, count), :]))
    copies = [pltpu.make_async_copy(*move, sems.at[i]) for i, move in enumerate(moves)]
    for copy in copies:
        copy.start()
    return copies


class Block:
    def __init__(self, sizes, table, b, q_all, g_all):
        self.sizes, self.table = sizes, table
        half, hdim = sizes.half, sizes.hdim
        self.own = pl.ds(pl.multiple_of(b * half, half), half)
        self.head = [slice(h * hdim, (h + 1) * hdim) for h in range(sizes.heads)]
        self.q_rows = jnp.concatenate([q_all[self.own, s] for s in self.head], axis=0)
        self.g_rows = jnp.concatenate([g_all[self.own, s] for s in self.head], axis=0)
        self.q_t = self.q_rows.T
        self.g_t = self.g_rows.T
        lane = lax.broadcasted_iota(jnp.int32, (1, sizes.rows), 1)
        self.position = table[sizes.at_own + b] * half + lax.rem(lane, half)
        start = jnp.zeros_like(self.position)
        for d in range(sizes.docs):
            end = table[sizes.at_ends + d]
            start = jnp.where(end <= self.position, jnp.maximum(start, end), start)
        self.start = start
        self.low = table[sizes.at_low + b]
        self.high = table[sizes.at_high + b]
        self.steps = lax.div(self.high - self.low + sizes.per_tile - 1, sizes.per_tile)

    def tile(self, i, k_all, v_all):
        sizes, half = self.sizes, self.sizes.half
        k_at, v_at, keys = [], [], []
        inside = lax.broadcasted_iota(jnp.int32, (half, 1), 0)
        for u in range(sizes.per_tile):
            rank = self.low + i * sizes.per_tile + u
            held = jnp.minimum(rank, self.high - 1)
            k_at.append(pl.ds(pl.multiple_of(self.table[sizes.at_key + held], half), half))
            v_at.append(pl.ds(pl.multiple_of(self.table[sizes.at_value + held], half), half))
            first = jnp.where(rank < self.high, self.table[sizes.at_block + held] * half, FAR)
            keys.append(first + inside)
        key = jnp.concatenate(keys, axis=0)
        k_tile = jnp.concatenate([k_all[p, :] for p in k_at], axis=0)
        v_tile = jnp.concatenate([v_all[p, :] for p in v_at], axis=0)
        s_t = jnp.dot(k_tile, self.q_t, preferred_element_type=jnp.float32)
        allowed = (key >= self.start) & (key <= self.position)
        e_t = jnp.where(allowed, jnp.exp2(s_t * (sizes.scale * LOG2E)), 0.0)
        return k_at, v_at, k_tile, v_tile, e_t

    def put(self, ref, value_t):
        rows = value_t.T.astype(ref.dtype)
        for h, s in enumerate(self.head):
            ref[self.own, s] = rows[h * self.sizes.half : (h + 1) * self.sizes.half, :]


def transposed_product(tile, weights):
    dims = (((0,), (0,)), ((), ()))
    return lax.dot_general(tile, weights, dims, preferred_element_type=jnp.float32)


def forward_kernel(sizes, table, *refs):
    pieces, refs = refs[:-9], refs[-9:]
    out_ref, stats_ref, q_all, g_all, k_all, v_all, out_t, totals, sems = refs
    copies = loaded(sizes, pieces, q_all, g_all, k_all, v_all, sems)
    for copy in copies:
        copy.wait()

    def one_block(b, carry):
        block = Block(sizes, table, b, q_all, g_all)
        out_t[...] = jnp.zeros_like(out_t)
        totals[...] = jnp.zeros_like(totals)

        def step(i, inner):
            _, _, _, v_tile, e_t = block.tile(i, k_all, v_all)
            totals[...] += jnp.sum(e_t.reshape(sizes.tile // 8, 8, sizes.rows), axis=0)
            out_t[...] += transposed_product(v_tile, e_t.astype(jnp.bfloat16))
            return inner

        lax.fori_loop(0, block.steps, step, 0)
        o_t = out_t[...]
        total = jnp.sum(totals[...], axis=0, keepdims=True)
        row_dot = jnp.sum(block.g_t.astype(jnp.float32) * o_t, axis=0, keepdims=True)
        stats_ref[b] = jnp.concatenate([total, row_dot], axis=0)
        block.put(out_ref, o_t)
        return carry

    lax.fori_loop(0, sizes.queries, one_block, 0)


def backward_kernel(sizes, table, *refs):
    pieces, refs = refs[: -13 - GROUP], refs[-13 - GROUP :]
    stats_refs, refs = refs[:GROUP], refs[GROUP:]
    dq_ref, dk_own, dk_other, dv_own, dv_other = refs[:5]
    q_all, g_all, k_all, v_all, dk_acc, dv_acc, dq_t, sems = refs[5:]
    half = sizes.half
    copies = loaded(sizes, pieces, q_all, g_all, k_all, v_all, sems)

    def clear(i, carry):
        at = pl.ds(pl.multiple_of(i * 256, 256), 256)
        dk_acc[at, :] = jnp.zeros((256, sizes.hdim), jnp.float32)
        dv_acc[at, :] = jnp.zeros((256, sizes.hdim), jnp.float32)
        return carry

    lax.fori_loop(0, sizes.keys // 256, clear, 0)
    for copy in copies:
        copy.wait()

    def one_block(b, carry):
        block = Block(sizes, table, b, q_all, g_all)
        dq_t[...] = jnp.zeros_like(dq_t)
        stats = stats_refs[0][b]
        for i in range(1, GROUP):
            stats = stats + stats_refs[i][lax.rem(b + sizes.queries - 2 * i, sizes.queries)]
        inverse = 1.0 / stats[0:1, :]
        row_dot = stats[1:2, :] * inverse

        def step(i, inner):
            k_at, v_at, k_tile, v_tile, e_t = block.tile(i, k_all, v_all)
            dp_t = jnp.dot(v_tile, block.g_t, preferred_element_type=jnp.float32)
            p_t = e_t * inverse
            ds_t = (p_t * (dp_t - row_dot)).astype(jnp.bfloat16)
            p_b = p_t.astype(jnp.bfloat16)
            dq_t[...] += transposed_product(k_tile, ds_t)
            dk = jnp.dot(ds_t, block.q_rows, preferred_element_type=jnp.float32)
            dv = jnp.dot(p_b, block.g_rows, preferred_element_type=jnp.float32)
            for u in range(sizes.per_tile):
                dk_acc[k_at[u], :] += dk[u * half : (u + 1) * half, :]
                dv_acc[v_at[u], :] += dv[u * half : (u + 1) * half, :]
            return inner

        lax.fori_loop(0, block.steps, step, 0)
        block.put(dq_ref, dq_t[...] * sizes.scale)
        return carry

    lax.fori_loop(0, sizes.queries, one_block, 0)

    def finish(i, carry):
        at = pl.ds(pl.multiple_of(i * 256, 256), 256)
        far = pl.ds(pl.multiple_of(sizes.keys // 2 + i * 256, 256), 256)
        dk_own[at, :] = (dk_acc[at, :] * sizes.scale).astype(jnp.bfloat16)
        dk_other[at, :] = (dk_acc[far, :] * sizes.scale).astype(jnp.bfloat16)
        dv_own[at, :] = dv_acc[at, :].astype(jnp.bfloat16)
        dv_other[at, :] = dv_acc[far, :].astype(jnp.bfloat16)
        return carry

    lax.fori_loop(0, sizes.keys // 512, finish, 0)


VMEM_SPEC = pl.BlockSpec(memory_space=pltpu.VMEM)
SMEM_SPEC = pl.BlockSpec(memory_space=pltpu.SMEM)
HBM_SPEC = pl.BlockSpec(memory_space=pltpu.HBM)


def held_arrays(sizes):
    wide = pltpu.VMEM((GROUP * sizes.tokens, sizes.width), jnp.bfloat16)
    narrow = pltpu.VMEM((sizes.keys, sizes.hdim), jnp.bfloat16)
    return [wide, wide, narrow, narrow]


def cost(sizes, products):
    pairs = sizes.keys * sizes.queries * sizes.rows // 4
    return pl.CostEstimate(
        flops=2 * products * sizes.hdim * pairs, bytes_accessed=6 << 20, transcendentals=pairs
    )


def forward(sizes, table, pieces):
    wide = jax.ShapeDtypeStruct((GROUP * sizes.tokens, sizes.width), jnp.bfloat16)
    return pl.pallas_call(
        functools.partial(forward_kernel, sizes),
        out_shape=(wide, jax.ShapeDtypeStruct((sizes.queries, 2, sizes.rows), jnp.float32)),
        in_specs=[SMEM_SPEC] + [HBM_SPEC] * len(pieces),
        out_specs=(VMEM_SPEC, VMEM_SPEC),
        scratch_shapes=held_arrays(sizes)
        + [
            pltpu.VMEM((sizes.hdim, sizes.rows), jnp.float32),
            pltpu.VMEM((8, sizes.rows), jnp.float32),
            pltpu.SemaphoreType.DMA((len(pieces) + GROUP,)),
        ],
        compiler_params=pltpu.CompilerParams(vmem_limit_bytes=24 * 1024 * 1024),
        cost_estimate=cost(sizes, 2),
        name="forward",
    )(table, *pieces)


def backward(sizes, table, pieces, stats):
    wide = jax.ShapeDtypeStruct((GROUP * sizes.tokens, sizes.width), jnp.bfloat16)
    term = jax.ShapeDtypeStruct((sizes.keys // 2, sizes.hdim), jnp.bfloat16)
    return pl.pallas_call(
        functools.partial(backward_kernel, sizes),
        out_shape=(wide, term, term, term, term),
        in_specs=[SMEM_SPEC] + [HBM_SPEC] * len(pieces) + [VMEM_SPEC] * GROUP,
        out_specs=(VMEM_SPEC,) * 5,
        scratch_shapes=held_arrays(sizes)
        + [
            pltpu.VMEM((sizes.keys, sizes.hdim), jnp.float32),
            pltpu.VMEM((sizes.keys, sizes.hdim), jnp.float32),
            pltpu.VMEM((sizes.hdim, sizes.rows), jnp.float32),
            pltpu.SemaphoreType.DMA((len(pieces) + GROUP,)),
        ],
        compiler_params=pltpu.CompilerParams(vmem_limit_bytes=32 * 1024 * 1024),
        cost_estimate=cost(sizes, 6),
        name="backward",
    )(table, *pieces, *stats)


def index_table(sizes, pair_order, doc_lengths, z, y, x, core):
    devices = pair_order.shape[0]
    device = jnp.arange(devices, dtype=jnp.int32)
    far_core, far_y = lax.rem(device % 2 + core, 2), lax.rem(device // 8 % 2 + y, 2)
    k_row = (far_core * 16 + far_y * 8 + device // 16) * sizes.tokens
    v_row = (far_core * 16 + device // 16 * 2 + far_y) * sizes.tokens
    mirrored = 2 * devices - 1 - pair_order
    block = jnp.concatenate([pair_order, mirrored])
    k_row = jnp.concatenate([k_row, k_row + sizes.half])
    v_row = jnp.concatenate([v_row, v_row + sizes.half])
    local = device // 2 % 4 == x
    local = jnp.concatenate([local, local])
    rank = jnp.sum((local[None, :] & (block[None, :] < block[:, None])).astype(jnp.int32), axis=1)
    place = jnp.arange(sizes.local, dtype=jnp.int32)
    chosen = local[None, :] & (rank[None, :] == place[:, None])
    k_at = jnp.sum(jnp.where(chosen, k_row[None, :], 0), axis=1)
    v_at = jnp.sum(jnp.where(chosen, v_row[None, :], 0), axis=1)
    held = jnp.sum(jnp.where(chosen, block[None, :], 0), axis=1)
    docs = jnp.arange(sizes.docs, dtype=jnp.int32)
    ends = jnp.sum(jnp.where(docs[None, :] <= docs[:, None], doc_lengths[None, :], 0), axis=1)
    query = jnp.arange(sizes.queries, dtype=jnp.int32)
    owner = z * 16 + y * 8 + lax.rem(x + query // 2, 4) * 2 + core
    own = jnp.sum(jnp.where(owner[:, None] == device[None, :], pair_order[None, :], 0), axis=1)
    own = jnp.where(query % 2 == 0, own, 2 * devices - 1 - own)
    first = own * sizes.half
    start = jnp.max(jnp.where(ends[None, :] <= first[:, None], ends[None, :], 0), axis=1)
    low = jnp.sum((held[None, :] < (start // sizes.half)[:, None]).astype(jnp.int32), axis=1)
    high = jnp.sum((held[None, :] <= own[:, None]).astype(jnp.int32), axis=1)
    return jnp.concatenate([k_at, v_at, held, ends, own, low, high]).astype(jnp.int32)


def from_x(a, step):
    return lax.ppermute(a, "x", [((i + step) % 4, i) for i in range(4)])


def swap(a, axis):
    return lax.ppermute(a, axis, [(0, 1), (1, 0)])


def added(*terms):
    return sum(t.astype(jnp.float32) for t in terms).astype(jnp.bfloat16)


def over_z(a):
    return lax.all_to_all(a, "z", 0, 0, tiled=True)


def gathered_x(queries, grad_out):
    both = jnp.concatenate([queries, grad_out], axis=0)
    pieces = [both]
    for step in (1, 2, 3):
        pieces.append(from_x(both, step))
    return pieces


def gathered_keys(keys, values):
    values = jnp.concatenate([values, swap(values, "y")], axis=0)
    k_near = over_z(jnp.tile(keys, (8, 1)))
    v = over_z(jnp.tile(values, (8, 1)))
    k_far = swap(k_near, "y")
    return [k_near, k_far, swap(k_near, "core"), swap(k_far, "core"), v, swap(v, "core")]


def scattered_keys(own, other, tokens):
    n = 8 * tokens
    other = swap(other, "core")
    far = swap(added(own[n:], other[n:]), "y")
    column = over_z(added(own[:n], other[:n], far))
    column = column.reshape(8, tokens, -1).astype(jnp.float32)
    return jnp.sum(column, axis=0).astype(jnp.bfloat16)


def scattered_values(own, other, tokens):
    other = swap(other, "core")
    column = over_z(added(own, other))
    column = column.reshape(8, 2 * tokens, -1).astype(jnp.float32)
    column = jnp.sum(column, axis=0)
    far = swap(column[tokens:].astype(jnp.bfloat16), "y")
    return added(column[:tokens], far)


def summed_x(parts, tokens):
    part = [parts[i * tokens : (i + 1) * tokens] for i in range(GROUP)]
    received = [part[0]]
    for step in (1, 2, 3):
        received.append(from_x(part[(4 - step) % 4], step))
    return received


def shared_stats(stats):
    arrived = [stats]
    for step in (1, 2, 3):
        arrived.append(from_x(stats, step))
    return arrived


def grads_of(queries, keys, values, grad_out, pair_order, doc_lengths):
    tokens, hdim = keys.shape
    width = queries.shape[1]
    sizes = Sizes(tokens, width, hdim, pair_order.shape[0], doc_lengths.shape[0])
    spot = [lax.axis_index(a) for a in AXES]
    table = index_table(sizes, pair_order, doc_lengths, *spot)
    pieces = gathered_x(queries, grad_out) + gathered_keys(keys, values)
    pieces = [pltpu.with_memory_space_constraint(p, pltpu.HBM) for p in pieces]
    out_parts, stats = forward(sizes, table, pieces)
    stats = shared_stats(stats)
    out_parts = summed_x(out_parts, tokens)
    dq_parts, *terms = backward(sizes, table, pieces, stats)
    total = sum(stats[i][(8 - 2 * i) % 8 : (8 - 2 * i) % 8 + 2, 0, :] for i in range(GROUP))
    total = total.reshape(2, sizes.heads, sizes.half)
    total = jnp.swapaxes(total, 1, 2).reshape(tokens, sizes.heads, 1)
    out = sum(p.astype(jnp.float32) for p in out_parts).reshape(tokens, sizes.heads, hdim)
    out = (out / total).astype(jnp.bfloat16).reshape(tokens, width)
    query_grad = added(*summed_x(dq_parts, tokens))
    key_grad = scattered_keys(*terms[:2], tokens)
    value_grad = scattered_values(*terms[2:], tokens)
    return out, query_grad, key_grad, value_grad


def solution(mesh):
    torus = Mesh(mesh.devices.reshape(*DIMS, mesh.shape["dp"]), AXES + ("dp",))
    rows = P(DP_CTX, None)
    return jax.shard_map(
        grads_of,
        mesh=torus,
        in_specs=(rows, rows, rows, rows, P("dp"), P("dp")),
        out_specs=(rows, rows, rows, rows),
        check_vma=False,
    )
```

```python
import functools

import jax
import jax.numpy as jnp
from jax import lax
from jax.experimental import pallas as pl
from jax.experimental.pallas import tpu as pltpu
from jax.sharding import Mesh
from jax.sharding import PartitionSpec as P

DIMS = (8, 2, 4, 2)
AXES = ("z", "y", "x", "core")
DP_CTX = ("dp",) + AXES
GROUP = 4
LOG2E = 1.4426950408889634
FAR = 1 << 20


class Sizes:
    def __init__(self, tokens, width, hdim, devices, docs):
        self.half = tokens // 2
        self.tokens = tokens
        self.width = width
        self.hdim = hdim
        self.heads = width // hdim
        self.rows = self.half * self.heads
        self.docs = docs
        self.local = 2 * devices // GROUP
        self.keys = self.local * self.half
        self.queries = 2 * GROUP
        self.per_tile = 4
        self.tile = self.per_tile * self.half
        self.scale = hdim ** (-0.5)
        self.at_key = 0
        self.at_value = self.local
        self.at_block = 2 * self.local
        self.at_ends = 3 * self.local
        self.at_own = self.at_ends + docs
        self.at_low = self.at_own + self.queries
        self.at_high = self.at_low + self.queries


def loaded(sizes, pieces, q_all, g_all, k_all, v_all, sems):
    moves = []
    tokens = sizes.tokens
    for i, piece in enumerate(pieces[:GROUP]):
        at = pl.ds(i * tokens, tokens)
        moves.append((piece.at[pl.ds(0, tokens), :], q_all.at[at, :]))
        moves.append((piece.at[pl.ds(tokens, tokens), :], g_all.at[at, :]))
    for part, whole in ((pieces[GROUP:-2], k_all), (pieces[-2:], v_all)):
        for i, piece in enumerate(part):
            count = piece.shape[0]
            moves.append((piece, whole.at[pl.ds(i * count, count), :]))
    copies = [pltpu.make_async_copy(*move, sems.at[i]) for i, move in enumerate(moves)]
    for copy in copies:
        copy.start()
    return copies


class Block:
    def __init__(self, sizes, table, b, q_all, g_all):
        self.sizes, self.table = sizes, table
        half, hdim = sizes.half, sizes.hdim
        self.own = pl.ds(pl.multiple_of(b * half, half), half)
        self.head = [slice(h * hdim, (h + 1) * hdim) for h in range(sizes.heads)]
        self.q_rows = jnp.concatenate([q_all[self.own, s] for s in self.head], axis=0)
        self.g_rows = jnp.concatenate([g_all[self.own, s] for s in self.head], axis=0)
        self.q_t = self.q_rows.T
        self.g_t = self.g_rows.T
        lane = lax.broadcasted_iota(jnp.int32, (1, sizes.rows), 1)
        self.position = table[sizes.at_own + b] * half + lax.rem(lane, half)
        start = jnp.zeros_like(self.position)
        for d in range(sizes.docs):
            end = table[sizes.at_ends + d]
            start = jnp.where(end <= self.position, jnp.maximum(start, end), start)
        self.start = start
        self.block = table[sizes.at_own + b]
        last = self.block * half + half - 1
        self.last_start = jnp.int32(0)
        for d in range(sizes.docs):
            end = table[sizes.at_ends + d]
            self.last_start = jnp.where(end <= last, jnp.maximum(self.last_start, end), self.last_start)
        self.low = table[sizes.at_low + b]
        self.high = table[sizes.at_high + b]
        self.steps = lax.div(self.high - self.low + sizes.per_tile - 1, sizes.per_tile)

    def whole(self, i):
        sizes, table = self.sizes, self.table
        first = self.low + i * sizes.per_tile
        last = jnp.minimum(first + sizes.per_tile, self.high) - 1
        inside = table[sizes.at_block + first] * sizes.half >= self.last_start
        past = table[sizes.at_block + last] < self.block
        return inside & past & (first + sizes.per_tile <= self.high)

    def each(self, step):
        def one(i, carry):
            whole = self.whole(i)
            pl.when(whole)(lambda: step(i, False))
            pl.when(jnp.logical_not(whole))(lambda: step(i, True))
            return carry

        lax.fori_loop(0, self.steps, one, 0)

    def tile(self, i, k_all, v_all, masked):
        sizes, half = self.sizes, self.sizes.half
        k_at, v_at, keys = [], [], []
        inside = lax.broadcasted_iota(jnp.int32, (half, 1), 0)
        for u in range(sizes.per_tile):
            rank = self.low + i * sizes.per_tile + u
            held = jnp.minimum(rank, self.high - 1)
            k_at.append(pl.ds(pl.multiple_of(self.table[sizes.at_key + held], half), half))
            v_at.append(pl.ds(pl.multiple_of(self.table[sizes.at_value + held], half), half))
            first = jnp.where(rank < self.high, self.table[sizes.at_block + held] * half, FAR)
            keys.append(first + inside)
        key = jnp.concatenate(keys, axis=0)
        k_tile = jnp.concatenate([k_all[p, :] for p in k_at], axis=0)
        v_tile = jnp.concatenate([v_all[p, :] for p in v_at], axis=0)
        s_t = jnp.dot(k_tile, self.q_t, preferred_element_type=jnp.float32)
        e_t = jnp.exp2(s_t * (sizes.scale * LOG2E))
        if masked:
            e_t = jnp.where((key >= self.start) & (key <= self.position), e_t, 0.0)
        return k_at, v_at, k_tile, v_tile, e_t

    def put(self, ref, value_t):
        rows = value_t.T.astype(ref.dtype)
        for h, s in enumerate(self.head):
            ref[self.own, s] = rows[h * self.sizes.half : (h + 1) * self.sizes.half, :]


def transposed_product(tile, weights):
    dims = (((0,), (0,)), ((), ()))
    return lax.dot_general(tile, weights, dims, preferred_element_type=jnp.float32)


def forward_kernel(sizes, table, *refs):
    pieces, refs = refs[:-9], refs[-9:]
    out_ref, stats_ref, q_all, g_all, k_all, v_all, out_t, totals, sems = refs
    copies = loaded(sizes, pieces, q_all, g_all, k_all, v_all, sems)
    for copy in copies:
        copy.wait()

    def one_block(b, carry):
        block = Block(sizes, table, b, q_all, g_all)
        out_t[...] = jnp.zeros_like(out_t)
        totals[...] = jnp.zeros_like(totals)

        def step(i, masked):
            _, _, _, v_tile, e_t = block.tile(i, k_all, v_all, masked)
            totals[...] += jnp.sum(e_t.reshape(sizes.tile // 8, 8, sizes.rows), axis=0)
            out_t[...] += transposed_product(v_tile, e_t.astype(jnp.bfloat16))

        block.each(step)
        o_t = out_t[...]
        total = jnp.sum(totals[...], axis=0, keepdims=True)
        row_dot = jnp.sum(block.g_t.astype(jnp.float32) * o_t, axis=0, keepdims=True)
        stats_ref[b] = jnp.concatenate([total, row_dot], axis=0)
        block.put(out_ref, o_t)
        return carry

    lax.fori_loop(0, sizes.queries, one_block, 0)


def backward_kernel(sizes, table, *refs):
    pieces, refs = refs[: -13 - GROUP], refs[-13 - GROUP :]
    stats_refs, refs = refs[:GROUP], refs[GROUP:]
    dq_ref, dk_own, dk_other, dv_own, dv_other = refs[:5]
    q_all, g_all, k_all, v_all, dk_acc, dv_acc, dq_t, sems = refs[5:]
    half = sizes.half
    copies = loaded(sizes, pieces, q_all, g_all, k_all, v_all, sems)

    def clear(i, carry):
        at = pl.ds(pl.multiple_of(i * 256, 256), 256)
        dk_acc[at, :] = jnp.zeros((256, sizes.hdim), jnp.float32)
        dv_acc[at, :] = jnp.zeros((256, sizes.hdim), jnp.float32)
        return carry

    lax.fori_loop(0, sizes.keys // 256, clear, 0)
    for copy in copies:
        copy.wait()

    def one_block(b, carry):
        block = Block(sizes, table, b, q_all, g_all)
        dq_t[...] = jnp.zeros_like(dq_t)
        stats = stats_refs[0][b]
        for i in range(1, GROUP):
            stats = stats + stats_refs[i][lax.rem(b + sizes.queries - 2 * i, sizes.queries)]
        inverse = 1.0 / stats[0:1, :]
        row_dot = stats[1:2, :] * inverse

        def step(i, masked):
            k_at, v_at, k_tile, v_tile, e_t = block.tile(i, k_all, v_all, masked)
            dp_t = jnp.dot(v_tile, block.g_t, preferred_element_type=jnp.float32)
            p_t = e_t * inverse
            ds_t = (p_t * (dp_t - row_dot)).astype(jnp.bfloat16)
            p_b = p_t.astype(jnp.bfloat16)
            dq_t[...] += transposed_product(k_tile, ds_t)
            dk = jnp.dot(ds_t, block.q_rows, preferred_element_type=jnp.float32)
            dv = jnp.dot(p_b, block.g_rows, preferred_element_type=jnp.float32)
            for u in range(sizes.per_tile):
                dk_acc[k_at[u], :] += dk[u * half : (u + 1) * half, :]
                dv_acc[v_at[u], :] += dv[u * half : (u + 1) * half, :]

        block.each(step)
        block.put(dq_ref, dq_t[...] * sizes.scale)
        return carry

    lax.fori_loop(0, sizes.queries, one_block, 0)

    def finish(i, carry):
        at = pl.ds(pl.multiple_of(i * 256, 256), 256)
        far = pl.ds(pl.multiple_of(sizes.keys // 2 + i * 256, 256), 256)
        dk_own[at, :] = (dk_acc[at, :] * sizes.scale).astype(jnp.bfloat16)
        dk_other[at, :] = (dk_acc[far, :] * sizes.scale).astype(jnp.bfloat16)
        dv_own[at, :] = dv_acc[at, :].astype(jnp.bfloat16)
        dv_other[at, :] = dv_acc[far, :].astype(jnp.bfloat16)
        return carry

    lax.fori_loop(0, sizes.keys // 512, finish, 0)


VMEM_SPEC = pl.BlockSpec(memory_space=pltpu.VMEM)
SMEM_SPEC = pl.BlockSpec(memory_space=pltpu.SMEM)
HBM_SPEC = pl.BlockSpec(memory_space=pltpu.HBM)


def held_arrays(sizes):
    wide = pltpu.VMEM((GROUP * sizes.tokens, sizes.width), jnp.bfloat16)
    narrow = pltpu.VMEM((sizes.keys, sizes.hdim), jnp.bfloat16)
    return [wide, wide, narrow, narrow]


def cost(sizes, products):
    pairs = sizes.keys * sizes.queries * sizes.rows // 4
    return pl.CostEstimate(
        flops=2 * products * sizes.hdim * pairs, bytes_accessed=6 << 20, transcendentals=pairs
    )


def forward(sizes, table, pieces):
    wide = jax.ShapeDtypeStruct((GROUP * sizes.tokens, sizes.width), jnp.bfloat16)
    return pl.pallas_call(
        functools.partial(forward_kernel, sizes),
        out_shape=(wide, jax.ShapeDtypeStruct((sizes.queries, 2, sizes.rows), jnp.float32)),
        in_specs=[SMEM_SPEC] + [HBM_SPEC] * len(pieces),
        out_specs=(VMEM_SPEC, VMEM_SPEC),
        scratch_shapes=held_arrays(sizes)
        + [
            pltpu.VMEM((sizes.hdim, sizes.rows), jnp.float32),
            pltpu.VMEM((8, sizes.rows), jnp.float32),
            pltpu.SemaphoreType.DMA((len(pieces) + GROUP,)),
        ],
        compiler_params=pltpu.CompilerParams(vmem_limit_bytes=24 * 1024 * 1024),
        cost_estimate=cost(sizes, 2),
        name="forward",
    )(table, *pieces)


def backward(sizes, table, pieces, stats):
    wide = jax.ShapeDtypeStruct((GROUP * sizes.tokens, sizes.width), jnp.bfloat16)
    term = jax.ShapeDtypeStruct((sizes.keys // 2, sizes.hdim), jnp.bfloat16)
    return pl.pallas_call(
        functools.partial(backward_kernel, sizes),
        out_shape=(wide, term, term, term, term),
        in_specs=[SMEM_SPEC] + [HBM_SPEC] * len(pieces) + [VMEM_SPEC] * GROUP,
        out_specs=(VMEM_SPEC,) * 5,
        scratch_shapes=held_arrays(sizes)
        + [
            pltpu.VMEM((sizes.keys, sizes.hdim), jnp.float32),
            pltpu.VMEM((sizes.keys, sizes.hdim), jnp.float32),
            pltpu.VMEM((sizes.hdim, sizes.rows), jnp.float32),
            pltpu.SemaphoreType.DMA((len(pieces) + GROUP,)),
        ],
        compiler_params=pltpu.CompilerParams(vmem_limit_bytes=32 * 1024 * 1024),
        cost_estimate=cost(sizes, 6),
        name="backward",
    )(table, *pieces, *stats)


def index_table(sizes, pair_order, doc_lengths, z, y, x, core):
    devices = pair_order.shape[0]
    device = jnp.arange(devices, dtype=jnp.int32)
    far_core, far_y = lax.rem(device % 2 + core, 2), lax.rem(device // 8 % 2 + y, 2)
    k_row = (far_core * 16 + far_y * 8 + device // 16) * sizes.tokens
    v_row = (far_core * 16 + lax.rem(device // 16 - z + 8, 8) * 2 + far_y) * sizes.tokens
    mirrored = 2 * devices - 1 - pair_order
    block = jnp.concatenate([pair_order, mirrored])
    k_row = jnp.concatenate([k_row, k_row + sizes.half])
    v_row = jnp.concatenate([v_row, v_row + sizes.half])
    local = device // 2 % 4 == x
    local = jnp.concatenate([local, local])
    rank = jnp.sum((local[None, :] & (block[None, :] < block[:, None])).astype(jnp.int32), axis=1)
    place = jnp.arange(sizes.local, dtype=jnp.int32)
    chosen = local[None, :] & (rank[None, :] == place[:, None])
    k_at = jnp.sum(jnp.where(chosen, k_row[None, :], 0), axis=1)
    v_at = jnp.sum(jnp.where(chosen, v_row[None, :], 0), axis=1)
    held = jnp.sum(jnp.where(chosen, block[None, :], 0), axis=1)
    docs = jnp.arange(sizes.docs, dtype=jnp.int32)
    ends = jnp.sum(jnp.where(docs[None, :] <= docs[:, None], doc_lengths[None, :], 0), axis=1)
    query = jnp.arange(sizes.queries, dtype=jnp.int32)
    owner = z * 16 + y * 8 + lax.rem(x + query // 2, 4) * 2 + core
    own = jnp.sum(jnp.where(owner[:, None] == device[None, :], pair_order[None, :], 0), axis=1)
    own = jnp.where(query % 2 == 0, own, 2 * devices - 1 - own)
    first = own * sizes.half
    start = jnp.max(jnp.where(ends[None, :] <= first[:, None], ends[None, :], 0), axis=1)
    low = jnp.sum((held[None, :] < (start // sizes.half)[:, None]).astype(jnp.int32), axis=1)
    high = jnp.sum((held[None, :] <= own[:, None]).astype(jnp.int32), axis=1)
    return jnp.concatenate([k_at, v_at, held, ends, own, low, high]).astype(jnp.int32)


def from_x(a, step):
    return lax.ppermute(a, "x", [((i + step) % 4, i) for i in range(4)])


def swap(a, axis):
    return lax.ppermute(a, axis, [(0, 1), (1, 0)])


def added(*terms):
    return sum(t.astype(jnp.float32) for t in terms).astype(jnp.bfloat16)


def over_z(a):
    return lax.all_to_all(a, "z", 0, 0, tiled=True)


def from_z(a, step):
    return lax.ppermute(a, "z", [((i + step) % 8, i) for i in range(8)])


def gathered_x(queries, grad_out):
    both = jnp.concatenate([queries, grad_out], axis=0)
    pieces = [both]
    for step in (1, 2, 3):
        pieces.append(from_x(both, step))
    return pieces


def gathered_keys(keys, values):
    values = jnp.concatenate([values, swap(values, "y")], axis=0)
    k_near = over_z(jnp.tile(keys, (8, 1)))
    v = [values]
    for step in range(1, 8):
        v.append(from_z(values, step))
    v = jnp.concatenate(v, axis=0)
    k_far = swap(k_near, "y")
    return [k_near, k_far, swap(k_near, "core"), swap(k_far, "core"), v, swap(v, "core")]


def scattered_keys(own, other, tokens):
    n = 8 * tokens
    other = swap(other, "core")
    far = swap(added(own[n:], other[n:]), "y")
    column = over_z(added(own[:n], other[:n], far))
    column = column.reshape(8, tokens, -1).astype(jnp.float32)
    return jnp.sum(column, axis=0).astype(jnp.bfloat16)


def scattered_values(own, other, tokens):
    other = swap(other, "core")
    n = 2 * tokens
    parts = [added(own[i * n : (i + 1) * n], other[i * n : (i + 1) * n]) for i in range(8)]
    column = parts[0].astype(jnp.float32)
    for step in range(1, 8):
        arrived = from_z(parts[8 - step], step)
        column = column + arrived.astype(jnp.float32)
    far = swap(column[tokens:].astype(jnp.bfloat16), "y")
    return added(column[:tokens], far)


def summed_x(parts, tokens):
    part = [parts[i * tokens : (i + 1) * tokens] for i in range(GROUP)]
    received = [part[0]]
    for step in (1, 2, 3):
        received.append(from_x(part[(4 - step) % 4], step))
    return received


def shared_stats(stats):
    arrived = [stats]
    for step in (1, 2, 3):
        arrived.append(from_x(stats, step))
    return arrived


def grads_of(queries, keys, values, grad_out, pair_order, doc_lengths):
    tokens, hdim = keys.shape
    width = queries.shape[1]
    sizes = Sizes(tokens, width, hdim, pair_order.shape[0], doc_lengths.shape[0])
    spot = [lax.axis_index(a) for a in AXES]
    table = index_table(sizes, pair_order, doc_lengths, *spot)
    pieces = gathered_x(queries, grad_out) + gathered_keys(keys, values)
    pieces = [pltpu.with_memory_space_constraint(p, pltpu.HBM) for p in pieces]
    out_parts, stats = forward(sizes, table, pieces)
    stats = shared_stats(stats)
    out_parts = summed_x(out_parts, tokens)
    dq_parts, *terms = backward(sizes, table, pieces, stats)
    total = sum(stats[i][(8 - 2 * i) % 8 : (8 - 2 * i) % 8 + 2, 0, :] for i in range(GROUP))
    total = total.reshape(2, sizes.heads, sizes.half)
    total = jnp.swapaxes(total, 1, 2).reshape(tokens, sizes.heads, 1)
    out = sum(p.astype(jnp.float32) for p in out_parts).reshape(tokens, sizes.heads, hdim)
    out = (out / total).astype(jnp.bfloat16).reshape(tokens, width)
    query_grad = added(*summed_x(dq_parts, tokens))
    key_grad = scattered_keys(*terms[:2], tokens)
    value_grad = scattered_values(*terms[2:], tokens)
    return out, query_grad, key_grad, value_grad


def solution(mesh):
    torus = Mesh(mesh.devices.reshape(*DIMS, mesh.shape["dp"]), AXES + ("dp",))
    rows = P(DP_CTX, None)
    return jax.shard_map(
        grads_of,
        mesh=torus,
        in_specs=(rows, rows, rows, rows, P("dp"), P("dp")),
        out_specs=(rows, rows, rows, rows),
        check_vma=False,
    )
```

```python
import functools

import jax
import jax.numpy as jnp
from jax import lax
from jax.experimental import pallas as pl
from jax.experimental.pallas import tpu as pltpu
from jax.sharding import Mesh
from jax.sharding import PartitionSpec as P

DIMS = (8, 2, 4, 2)
AXES = ("z", "y", "x", "core")
DP_CTX = ("dp",) + AXES
GROUP = 4
LOG2E = 1.4426950408889634
FAR = 1 << 20


class Sizes:
    def __init__(self, tokens, width, hdim, devices, docs):
        self.half = tokens // 2
        self.tokens = tokens
        self.width = width
        self.hdim = hdim
        self.heads = width // hdim
        self.rows = self.half * self.heads
        self.docs = docs
        self.local = 2 * devices // GROUP
        self.keys = self.local * self.half
        self.queries = 2 * GROUP
        self.per_tile = 4
        self.tile = self.per_tile * self.half
        self.scale = hdim ** (-0.5)
        self.at_key = 0
        self.at_block = self.local
        self.at_ends = 2 * self.local
        self.at_own = self.at_ends + docs
        self.at_low = self.at_own + self.queries
        self.at_high = self.at_low + self.queries


def loaded(sizes, pieces, q_all, g_all, kv_all, sems):
    moves = []
    tokens = sizes.tokens
    for i, piece in enumerate(pieces[:GROUP]):
        at = pl.ds(i * tokens, tokens)
        moves.append((piece.at[pl.ds(0, tokens), :], q_all.at[at, :]))
        moves.append((piece.at[pl.ds(tokens, tokens), :], g_all.at[at, :]))
    for i, piece in enumerate(pieces[GROUP:]):
        count = piece.shape[0]
        moves.append((piece, kv_all.at[pl.ds(i * count, count), :]))
    copies = [pltpu.make_async_copy(*move, sems.at[i]) for i, move in enumerate(moves)]
    for copy in copies:
        copy.start()
    return copies


class Block:
    def __init__(self, sizes, table, b, q_all, g_all):
        self.sizes, self.table = sizes, table
        half, hdim = sizes.half, sizes.hdim
        self.own = pl.ds(pl.multiple_of(b * half, half), half)
        self.head = [slice(h * hdim, (h + 1) * hdim) for h in range(sizes.heads)]
        self.q_rows = jnp.concatenate([q_all[self.own, s] for s in self.head], axis=0)
        self.g_rows = jnp.concatenate([g_all[self.own, s] for s in self.head], axis=0)
        self.q_t = self.q_rows.T
        self.g_t = self.g_rows.T
        lane = lax.broadcasted_iota(jnp.int32, (1, sizes.rows), 1)
        self.position = table[sizes.at_own + b] * half + lax.rem(lane, half)
        start = jnp.zeros_like(self.position)
        for d in range(sizes.docs):
            end = table[sizes.at_ends + d]
            start = jnp.where(end <= self.position, jnp.maximum(start, end), start)
        self.start = start
        self.block = table[sizes.at_own + b]
        last = self.block * half + half - 1
        self.last_start = jnp.int32(0)
        for d in range(sizes.docs):
            end = table[sizes.at_ends + d]
            self.last_start = jnp.where(end <= last, jnp.maximum(self.last_start, end), self.last_start)
        self.low = table[sizes.at_low + b]
        self.high = table[sizes.at_high + b]
        self.steps = lax.div(self.high - self.low + sizes.per_tile - 1, sizes.per_tile)

    def whole(self, i):
        sizes, table = self.sizes, self.table
        first = self.low + i * sizes.per_tile
        last = jnp.minimum(first + sizes.per_tile, self.high) - 1
        inside = table[sizes.at_block + first] * sizes.half >= self.last_start
        past = table[sizes.at_block + last] < self.block
        return inside & past & (first + sizes.per_tile <= self.high)

    def each(self, step):
        def one(i, carry):
            whole = self.whole(i)
            pl.when(whole)(lambda: step(i, False))
            pl.when(jnp.logical_not(whole))(lambda: step(i, True))
            return carry

        lax.fori_loop(0, self.steps, one, 0)

    def tile(self, i, kv_all, masked):
        sizes, half, hdim = self.sizes, self.sizes.half, self.sizes.hdim
        places, keys = [], []
        inside = lax.broadcasted_iota(jnp.int32, (half, 1), 0)
        for u in range(sizes.per_tile):
            rank = self.low + i * sizes.per_tile + u
            held = jnp.minimum(rank, self.high - 1)
            places.append(pl.ds(pl.multiple_of(self.table[sizes.at_key + held], half), half))
            first = jnp.where(rank < self.high, self.table[sizes.at_block + held] * half, FAR)
            keys.append(first + inside)
        key = jnp.concatenate(keys, axis=0)
        k_tile = jnp.concatenate([kv_all[p, 0:hdim] for p in places], axis=0)
        v_tile = jnp.concatenate([kv_all[p, hdim : 2 * hdim] for p in places], axis=0)
        s_t = jnp.dot(k_tile, self.q_t, preferred_element_type=jnp.float32)
        e_t = jnp.exp2(s_t * (sizes.scale * LOG2E))
        if masked:
            e_t = jnp.where((key >= self.start) & (key <= self.position), e_t, 0.0)
        return places, k_tile, v_tile, e_t

    def put(self, ref, value_t):
        rows = value_t.T.astype(ref.dtype)
        for h, s in enumerate(self.head):
            ref[self.own, s] = rows[h * self.sizes.half : (h + 1) * self.sizes.half, :]


def transposed_product(tile, weights):
    dims = (((0,), (0,)), ((), ()))
    return lax.dot_general(tile, weights, dims, preferred_element_type=jnp.float32)


def forward_kernel(sizes, table, *refs):
    pieces, refs = refs[:-8], refs[-8:]
    out_ref, stats_ref, q_all, g_all, kv_all, out_t, totals, sems = refs
    copies = loaded(sizes, pieces, q_all, g_all, kv_all, sems)
    for copy in copies:
        copy.wait()

    def one_block(b, carry):
        block = Block(sizes, table, b, q_all, g_all)
        out_t[...] = jnp.zeros_like(out_t)
        totals[...] = jnp.zeros_like(totals)

        def step(i, masked):
            _, _, v_tile, e_t = block.tile(i, kv_all, masked)
            totals[...] += jnp.sum(e_t.reshape(sizes.tile // 8, 8, sizes.rows), axis=0)
            out_t[...] += transposed_product(v_tile, e_t.astype(jnp.bfloat16))

        block.each(step)
        o_t = out_t[...]
        total = jnp.sum(totals[...], axis=0, keepdims=True)
        row_dot = jnp.sum(block.g_t.astype(jnp.float32) * o_t, axis=0, keepdims=True)
        stats_ref[b] = jnp.concatenate([total, row_dot], axis=0)
        block.put(out_ref, o_t)
        return carry

    lax.fori_loop(0, sizes.queries, one_block, 0)


def backward_kernel(sizes, table, *refs):
    pieces, refs = refs[: -10 - GROUP], refs[-10 - GROUP :]
    stats_refs, refs = refs[:GROUP], refs[GROUP:]
    dq_ref, own_ref, other_ref, q_all, g_all, kv_all, dk_acc, dv_acc, dq_t, sems = refs
    half, hdim = sizes.half, sizes.hdim
    copies = loaded(sizes, pieces, q_all, g_all, kv_all, sems)

    def clear(i, carry):
        at = pl.ds(pl.multiple_of(i * 256, 256), 256)
        dk_acc[at, :] = jnp.zeros((256, sizes.hdim), jnp.float32)
        dv_acc[at, :] = jnp.zeros((256, sizes.hdim), jnp.float32)
        return carry

    lax.fori_loop(0, sizes.keys // 256, clear, 0)
    for copy in copies:
        copy.wait()

    def one_block(b, carry):
        block = Block(sizes, table, b, q_all, g_all)
        dq_t[...] = jnp.zeros_like(dq_t)
        stats = stats_refs[0][b]
        for i in range(1, GROUP):
            stats = stats + stats_refs[i][lax.rem(b + sizes.queries - 2 * i, sizes.queries)]
        inverse = 1.0 / stats[0:1, :]
        row_dot = stats[1:2, :] * inverse

        def step(i, masked):
            places, k_tile, v_tile, e_t = block.tile(i, kv_all, masked)
            dp_t = jnp.dot(v_tile, block.g_t, preferred_element_type=jnp.float32)
            p_t = e_t * inverse
            ds_t = (p_t * (dp_t - row_dot)).astype(jnp.bfloat16)
            p_b = p_t.astype(jnp.bfloat16)
            dq_t[...] += transposed_product(k_tile, ds_t)
            dk = jnp.dot(ds_t, block.q_rows, preferred_element_type=jnp.float32)
            dv = jnp.dot(p_b, block.g_rows, preferred_element_type=jnp.float32)
            for u, p in enumerate(places):
                dk_acc[p, :] += dk[u * half : (u + 1) * half, :]
                dv_acc[p, :] += dv[u * half : (u + 1) * half, :]

        block.each(step)
        block.put(dq_ref, dq_t[...] * sizes.scale)
        return carry

    lax.fori_loop(0, sizes.queries, one_block, 0)

    def finish(i, carry):
        at = pl.ds(pl.multiple_of(i * 256, 256), 256)
        far = pl.ds(pl.multiple_of(sizes.keys // 2 + i * 256, 256), 256)
        for ref, rows in ((own_ref, at), (other_ref, far)):
            ref[at, 0:hdim] = (dk_acc[rows, :] * sizes.scale).astype(jnp.bfloat16)
            ref[at, hdim : 2 * hdim] = dv_acc[rows, :].astype(jnp.bfloat16)
        return carry

    lax.fori_loop(0, sizes.keys // 512, finish, 0)


VMEM_SPEC = pl.BlockSpec(memory_space=pltpu.VMEM)
SMEM_SPEC = pl.BlockSpec(memory_space=pltpu.SMEM)
HBM_SPEC = pl.BlockSpec(memory_space=pltpu.HBM)


def held_arrays(sizes):
    wide = pltpu.VMEM((GROUP * sizes.tokens, sizes.width), jnp.bfloat16)
    return [wide, wide, pltpu.VMEM((sizes.keys, 2 * sizes.hdim), jnp.bfloat16)]


def cost(sizes, products):
    pairs = sizes.keys * sizes.queries * sizes.rows // 4
    return pl.CostEstimate(
        flops=2 * products * sizes.hdim * pairs, bytes_accessed=6 << 20, transcendentals=pairs
    )


def forward(sizes, table, pieces):
    wide = jax.ShapeDtypeStruct((GROUP * sizes.tokens, sizes.width), jnp.bfloat16)
    return pl.pallas_call(
        functools.partial(forward_kernel, sizes),
        out_shape=(wide, jax.ShapeDtypeStruct((sizes.queries, 2, sizes.rows), jnp.float32)),
        in_specs=[SMEM_SPEC] + [HBM_SPEC] * len(pieces),
        out_specs=(VMEM_SPEC, VMEM_SPEC),
        scratch_shapes=held_arrays(sizes)
        + [
            pltpu.VMEM((sizes.hdim, sizes.rows), jnp.float32),
            pltpu.VMEM((8, sizes.rows), jnp.float32),
            pltpu.SemaphoreType.DMA((len(pieces) + GROUP,)),
        ],
        compiler_params=pltpu.CompilerParams(vmem_limit_bytes=24 * 1024 * 1024),
        cost_estimate=cost(sizes, 2),
        name="forward",
    )(table, *pieces)


def backward(sizes, table, pieces, stats):
    wide = jax.ShapeDtypeStruct((GROUP * sizes.tokens, sizes.width), jnp.bfloat16)
    term = jax.ShapeDtypeStruct((sizes.keys // 2, 2 * sizes.hdim), jnp.bfloat16)
    return pl.pallas_call(
        functools.partial(backward_kernel, sizes),
        out_shape=(wide, term, term),
        in_specs=[SMEM_SPEC] + [HBM_SPEC] * len(pieces) + [VMEM_SPEC] * GROUP,
        out_specs=(VMEM_SPEC,) * 3,
        scratch_shapes=held_arrays(sizes)
        + [
            pltpu.VMEM((sizes.keys, sizes.hdim), jnp.float32),
            pltpu.VMEM((sizes.keys, sizes.hdim), jnp.float32),
            pltpu.VMEM((sizes.hdim, sizes.rows), jnp.float32),
            pltpu.SemaphoreType.DMA((len(pieces) + GROUP,)),
        ],
        compiler_params=pltpu.CompilerParams(vmem_limit_bytes=32 * 1024 * 1024),
        cost_estimate=cost(sizes, 6),
        name="backward",
    )(table, *pieces, *stats)


def index_table(sizes, pair_order, doc_lengths, z, y, x, core):
    devices = pair_order.shape[0]
    device = jnp.arange(devices, dtype=jnp.int32)
    far_core, far_y = lax.rem(device % 2 + core, 2), lax.rem(device // 8 % 2 + y, 2)
    row = (far_core * 16 + device // 16 * 2 + far_y) * sizes.tokens
    mirrored = 2 * devices - 1 - pair_order
    block = jnp.concatenate([pair_order, mirrored])
    row = jnp.concatenate([row, row + sizes.half])
    local = device // 2 % 4 == x
    local = jnp.concatenate([local, local])
    rank = jnp.sum((local[None, :] & (block[None, :] < block[:, None])).astype(jnp.int32), axis=1)
    place = jnp.arange(sizes.local, dtype=jnp.int32)
    chosen = local[None, :] & (rank[None, :] == place[:, None])
    address = jnp.sum(jnp.where(chosen, row[None, :], 0), axis=1)
    held = jnp.sum(jnp.where(chosen, block[None, :], 0), axis=1)
    docs = jnp.arange(sizes.docs, dtype=jnp.int32)
    ends = jnp.sum(jnp.where(docs[None, :] <= docs[:, None], doc_lengths[None, :], 0), axis=1)
    query = jnp.arange(sizes.queries, dtype=jnp.int32)
    owner = z * 16 + y * 8 + lax.rem(x + query // 2, 4) * 2 + core
    own = jnp.sum(jnp.where(owner[:, None] == device[None, :], pair_order[None, :], 0), axis=1)
    own = jnp.where(query % 2 == 0, own, 2 * devices - 1 - own)
    first = own * sizes.half
    start = jnp.max(jnp.where(ends[None, :] <= first[:, None], ends[None, :], 0), axis=1)
    low = jnp.sum((held[None, :] < (start // sizes.half)[:, None]).astype(jnp.int32), axis=1)
    high = jnp.sum((held[None, :] <= own[:, None]).astype(jnp.int32), axis=1)
    return jnp.concatenate([address, held, ends, own, low, high]).astype(jnp.int32)


def from_x(a, step):
    return lax.ppermute(a, "x", [((i + step) % 4, i) for i in range(4)])


def swap(a, axis):
    return lax.ppermute(a, axis, [(0, 1), (1, 0)])


def added(*terms):
    return sum(t.astype(jnp.float32) for t in terms).astype(jnp.bfloat16)


def over_z(a):
    return lax.all_to_all(a, "z", 0, 0, tiled=True)


def gathered_x(queries, grad_out):
    both = jnp.concatenate([queries, grad_out], axis=0)
    pieces = [both]
    for step in (1, 2, 3):
        pieces.append(from_x(both, step))
    return pieces


def gathered_keys(keys, values):
    kv = jnp.concatenate([keys, values], axis=1)
    pair = jnp.concatenate([kv, swap(kv, "y")], axis=0)
    near = over_z(jnp.tile(pair, (8, 1)))
    return [near, swap(near, "core")]


def scattered_keys(own, other, tokens):
    other = swap(other, "core")
    own, other = (a.reshape(8, 2, tokens, -1) for a in (own, other))
    far = swap(added(own[:, 1], other[:, 1]), "y")
    column = over_z(added(own[:, 0], other[:, 0], far))
    return jnp.sum(column.astype(jnp.float32), axis=0).astype(jnp.bfloat16)


def summed_x(first, second, tokens):
    totals = [a[:tokens].astype(jnp.float32) for a in (first, second)]
    for step in (1, 2, 3):
        at = slice((4 - step) * tokens, (5 - step) * tokens)
        arrived = from_x(jnp.concatenate([first[at], second[at]], axis=0), step)
        totals[0] = totals[0] + arrived[:tokens].astype(jnp.float32)
        totals[1] = totals[1] + arrived[tokens:].astype(jnp.float32)
    return totals


def shared_stats(stats):
    arrived = [stats]
    for step in (1, 2, 3):
        arrived.append(from_x(stats, step))
    return arrived


def grads_of(queries, keys, values, grad_out, pair_order, doc_lengths):
    tokens, hdim = keys.shape
    width = queries.shape[1]
    sizes = Sizes(tokens, width, hdim, pair_order.shape[0], doc_lengths.shape[0])
    spot = [lax.axis_index(a) for a in AXES]
    table = index_table(sizes, pair_order, doc_lengths, *spot)
    pieces = gathered_x(queries, grad_out) + gathered_keys(keys, values)
    pieces = [pltpu.with_memory_space_constraint(p, pltpu.HBM) for p in pieces]
    out_parts, stats = forward(sizes, table, pieces)
    stats = shared_stats(stats)
    dq_parts, *terms = backward(sizes, table, pieces, stats)
    total = sum(stats[i][(8 - 2 * i) % 8 : (8 - 2 * i) % 8 + 2, 0, :] for i in range(GROUP))
    total = total.reshape(2, sizes.heads, sizes.half)
    total = jnp.swapaxes(total, 1, 2).reshape(tokens, sizes.heads, 1)
    out, query_grad = summed_x(out_parts, dq_parts, tokens)
    out = out.reshape(tokens, sizes.heads, hdim) / total
    out = out.astype(jnp.bfloat16).reshape(tokens, width)
    grads = scattered_keys(*terms, tokens)
    return out, query_grad.astype(jnp.bfloat16), grads[:, :hdim], grads[:, hdim:]


def solution(mesh):
    torus = Mesh(mesh.devices.reshape(*DIMS, mesh.shape["dp"]), AXES + ("dp",))
    rows = P(DP_CTX, None)
    return jax.shard_map(
        grads_of,
        mesh=torus,
        in_specs=(rows, rows, rows, rows, P("dp"), P("dp")),
        out_specs=(rows, rows, rows, rows),
        check_vma=False,
    )
```

```python
import functools

import jax
import jax.numpy as jnp
from jax import lax
from jax.experimental import pallas as pl
from jax.experimental.pallas import tpu as pltpu
from jax.sharding import Mesh
from jax.sharding import PartitionSpec as P

DIMS = (8, 2, 4, 2)
AXES = ("z", "y", "x", "core")
DP_CTX = ("dp",) + AXES
GROUP = 4
LOG2E = 1.4426950408889634
FAR = 1 << 20


class Sizes:
    def __init__(self, tokens, width, hdim, devices, docs):
        self.half = tokens // 2
        self.tokens = tokens
        self.width = width
        self.hdim = hdim
        self.heads = width // hdim
        self.rows = self.half * self.heads
        self.docs = docs
        self.local = 2 * devices // GROUP
        self.keys = self.local * self.half
        self.queries = 2 * GROUP
        self.per_tile = 6
        self.tile = self.per_tile * self.half
        self.scale = hdim ** (-0.5)
        self.at_key = 0
        self.at_block = self.local
        self.at_ends = 2 * self.local
        self.at_own = self.at_ends + docs
        self.at_low = self.at_own + self.queries
        self.at_high = self.at_low + self.queries


def loaded(sizes, pieces, q_all, g_all, kv_all, sems):
    moves = []
    tokens = sizes.tokens
    for i, piece in enumerate(pieces[:GROUP]):
        at = pl.ds(i * tokens, tokens)
        moves.append((piece.at[pl.ds(0, tokens), :], q_all.at[at, :]))
        moves.append((piece.at[pl.ds(tokens, tokens), :], g_all.at[at, :]))
    for i, piece in enumerate(pieces[GROUP:]):
        count = piece.shape[0]
        moves.append((piece, kv_all.at[pl.ds(i * count, count), :]))
    copies = [pltpu.make_async_copy(*move, sems.at[i]) for i, move in enumerate(moves)]
    for copy in copies:
        copy.start()
    return copies


class Block:
    def __init__(self, sizes, table, b, q_all, g_all):
        self.sizes, self.table = sizes, table
        half, hdim = sizes.half, sizes.hdim
        self.own = pl.ds(pl.multiple_of(b * half, half), half)
        self.head = [slice(h * hdim, (h + 1) * hdim) for h in range(sizes.heads)]
        self.q_rows = jnp.concatenate([q_all[self.own, s] for s in self.head], axis=0)
        self.g_rows = jnp.concatenate([g_all[self.own, s] for s in self.head], axis=0)
        self.q_t = self.q_rows.T
        self.g_t = self.g_rows.T
        lane = lax.broadcasted_iota(jnp.int32, (1, sizes.rows), 1)
        self.position = table[sizes.at_own + b] * half + lax.rem(lane, half)
        start = jnp.zeros_like(self.position)
        for d in range(sizes.docs):
            end = table[sizes.at_ends + d]
            start = jnp.where(end <= self.position, jnp.maximum(start, end), start)
        self.start = start
        self.block = table[sizes.at_own + b]
        last = self.block * half + half - 1
        self.last_start = jnp.int32(0)
        for d in range(sizes.docs):
            end = table[sizes.at_ends + d]
            self.last_start = jnp.where(end <= last, jnp.maximum(self.last_start, end), self.last_start)
        self.low = table[sizes.at_low + b]
        self.high = table[sizes.at_high + b]
        self.steps = lax.div(self.high - self.low + sizes.per_tile - 1, sizes.per_tile)

    def whole(self, i):
        sizes, table = self.sizes, self.table
        first = self.low + i * sizes.per_tile
        last = jnp.minimum(first + sizes.per_tile, self.high) - 1
        inside = table[sizes.at_block + first] * sizes.half >= self.last_start
        past = table[sizes.at_block + last] < self.block
        return inside & past & (first + sizes.per_tile <= self.high)

    def each(self, step):
        def one(i, carry):
            whole = self.whole(i)
            pl.when(whole)(lambda: step(i, False))
            pl.when(jnp.logical_not(whole))(lambda: step(i, True))
            return carry

        lax.fori_loop(0, self.steps, one, 0)

    def tile(self, i, kv_all, masked):
        sizes, half, hdim = self.sizes, self.sizes.half, self.sizes.hdim
        places, keys = [], []
        inside = lax.broadcasted_iota(jnp.int32, (half, 1), 0)
        for u in range(sizes.per_tile):
            rank = self.low + i * sizes.per_tile + u
            held = jnp.minimum(rank, self.high - 1)
            places.append(pl.ds(pl.multiple_of(self.table[sizes.at_key + held], half), half))
            first = jnp.where(rank < self.high, self.table[sizes.at_block + held] * half, FAR)
            keys.append(first + inside)
        key = jnp.concatenate(keys, axis=0)
        k_tile = jnp.concatenate([kv_all[p, 0:hdim] for p in places], axis=0)
        v_tile = jnp.concatenate([kv_all[p, hdim : 2 * hdim] for p in places], axis=0)
        s_t = jnp.dot(k_tile, self.q_t, preferred_element_type=jnp.float32)
        e_t = jnp.exp2(s_t * (sizes.scale * LOG2E))
        if masked:
            e_t = jnp.where((key >= self.start) & (key <= self.position), e_t, 0.0)
        return places, k_tile, v_tile, e_t

    def put(self, ref, value_t):
        rows = value_t.T.astype(ref.dtype)
        for h, s in enumerate(self.head):
            ref[self.own, s] = rows[h * self.sizes.half : (h + 1) * self.sizes.half, :]


def transposed_product(tile, weights):
    dims = (((0,), (0,)), ((), ()))
    return lax.dot_general(tile, weights, dims, preferred_element_type=jnp.float32)


def forward_kernel(sizes, table, *refs):
    pieces, refs = refs[:-8], refs[-8:]
    out_ref, stats_ref, q_all, g_all, kv_all, out_t, totals, sems = refs
    copies = loaded(sizes, pieces, q_all, g_all, kv_all, sems)
    for copy in copies:
        copy.wait()

    def one_block(b, carry):
        block = Block(sizes, table, b, q_all, g_all)
        out_t[...] = jnp.zeros_like(out_t)
        totals[...] = jnp.zeros_like(totals)

        def step(i, masked):
            _, _, v_tile, e_t = block.tile(i, kv_all, masked)
            totals[...] += jnp.sum(e_t.reshape(sizes.tile // 8, 8, sizes.rows), axis=0)
            out_t[...] += transposed_product(v_tile, e_t.astype(jnp.bfloat16))

        block.each(step)
        o_t = out_t[...]
        total = jnp.sum(totals[...], axis=0, keepdims=True)
        row_dot = jnp.sum(block.g_t.astype(jnp.float32) * o_t, axis=0, keepdims=True)
        stats_ref[b] = jnp.concatenate([total, row_dot], axis=0)
        block.put(out_ref, o_t)
        return carry

    lax.fori_loop(0, sizes.queries, one_block, 0)


def backward_kernel(sizes, table, *refs):
    pieces, refs = refs[: -10 - GROUP], refs[-10 - GROUP :]
    stats_refs, refs = refs[:GROUP], refs[GROUP:]
    dq_ref, own_ref, other_ref, q_all, g_all, kv_all, dk_acc, dv_acc, dq_t, sems = refs
    half, hdim = sizes.half, sizes.hdim
    copies = loaded(sizes, pieces, q_all, g_all, kv_all, sems)

    def clear(i, carry):
        at = pl.ds(pl.multiple_of(i * 256, 256), 256)
        dk_acc[at, :] = jnp.zeros((256, sizes.hdim), jnp.float32)
        dv_acc[at, :] = jnp.zeros((256, sizes.hdim), jnp.float32)
        return carry

    lax.fori_loop(0, sizes.keys // 256, clear, 0)
    for copy in copies:
        copy.wait()

    def one_block(b, carry):
        block = Block(sizes, table, b, q_all, g_all)
        dq_t[...] = jnp.zeros_like(dq_t)
        stats = stats_refs[0][b]
        for i in range(1, GROUP):
            stats = stats + stats_refs[i][lax.rem(b + sizes.queries - 2 * i, sizes.queries)]
        inverse = 1.0 / stats[0:1, :]
        row_dot = stats[1:2, :] * inverse

        def step(i, masked):
            places, k_tile, v_tile, e_t = block.tile(i, kv_all, masked)
            dp_t = jnp.dot(v_tile, block.g_t, preferred_element_type=jnp.float32)
            p_t = e_t * inverse
            ds_t = (p_t * (dp_t - row_dot)).astype(jnp.bfloat16)
            p_b = p_t.astype(jnp.bfloat16)
            dq_t[...] += transposed_product(k_tile, ds_t)
            dk = jnp.dot(ds_t, block.q_rows, preferred_element_type=jnp.float32)
            dv = jnp.dot(p_b, block.g_rows, preferred_element_type=jnp.float32)
            for u, p in enumerate(places):
                dk_acc[p, :] += dk[u * half : (u + 1) * half, :]
                dv_acc[p, :] += dv[u * half : (u + 1) * half, :]

        block.each(step)
        block.put(dq_ref, dq_t[...] * sizes.scale)
        return carry

    lax.fori_loop(0, sizes.queries, one_block, 0)

    def finish(i, carry):
        at = pl.ds(pl.multiple_of(i * 256, 256), 256)
        far = pl.ds(pl.multiple_of(sizes.keys // 2 + i * 256, 256), 256)
        for ref, rows in ((own_ref, at), (other_ref, far)):
            ref[at, 0:hdim] = (dk_acc[rows, :] * sizes.scale).astype(jnp.bfloat16)
            ref[at, hdim : 2 * hdim] = dv_acc[rows, :].astype(jnp.bfloat16)
        return carry

    lax.fori_loop(0, sizes.keys // 512, finish, 0)


VMEM_SPEC = pl.BlockSpec(memory_space=pltpu.VMEM)
SMEM_SPEC = pl.BlockSpec(memory_space=pltpu.SMEM)
HBM_SPEC = pl.BlockSpec(memory_space=pltpu.HBM)


def held_arrays(sizes):
    wide = pltpu.VMEM((GROUP * sizes.tokens, sizes.width), jnp.bfloat16)
    return [wide, wide, pltpu.VMEM((sizes.keys, 2 * sizes.hdim), jnp.bfloat16)]


def cost(sizes, products):
    pairs = sizes.keys * sizes.queries * sizes.rows // 4
    return pl.CostEstimate(
        flops=2 * products * sizes.hdim * pairs, bytes_accessed=6 << 20, transcendentals=pairs
    )


def forward(sizes, table, pieces):
    wide = jax.ShapeDtypeStruct((GROUP * sizes.tokens, sizes.width), jnp.bfloat16)
    return pl.pallas_call(
        functools.partial(forward_kernel, sizes),
        out_shape=(wide, jax.ShapeDtypeStruct((sizes.queries, 2, sizes.rows), jnp.float32)),
        in_specs=[SMEM_SPEC] + [HBM_SPEC] * len(pieces),
        out_specs=(VMEM_SPEC, VMEM_SPEC),
        scratch_shapes=held_arrays(sizes)
        + [
            pltpu.VMEM((sizes.hdim, sizes.rows), jnp.float32),
            pltpu.VMEM((8, sizes.rows), jnp.float32),
            pltpu.SemaphoreType.DMA((len(pieces) + GROUP,)),
        ],
        compiler_params=pltpu.CompilerParams(vmem_limit_bytes=24 * 1024 * 1024),
        cost_estimate=cost(sizes, 2),
        name="forward",
    )(table, *pieces)


def backward(sizes, table, pieces, stats):
    wide = jax.ShapeDtypeStruct((GROUP * sizes.tokens, sizes.width), jnp.bfloat16)
    term = jax.ShapeDtypeStruct((sizes.keys // 2, 2 * sizes.hdim), jnp.bfloat16)
    return pl.pallas_call(
        functools.partial(backward_kernel, sizes),
        out_shape=(wide, term, term),
        in_specs=[SMEM_SPEC] + [HBM_SPEC] * len(pieces) + [VMEM_SPEC] * GROUP,
        out_specs=(VMEM_SPEC,) * 3,
        scratch_shapes=held_arrays(sizes)
        + [
            pltpu.VMEM((sizes.keys, sizes.hdim), jnp.float32),
            pltpu.VMEM((sizes.keys, sizes.hdim), jnp.float32),
            pltpu.VMEM((sizes.hdim, sizes.rows), jnp.float32),
            pltpu.SemaphoreType.DMA((len(pieces) + GROUP,)),
        ],
        compiler_params=pltpu.CompilerParams(vmem_limit_bytes=32 * 1024 * 1024),
        cost_estimate=cost(sizes, 6),
        name="backward",
    )(table, *pieces, *stats)


def index_table(sizes, pair_order, doc_lengths, z, y, x, core):
    devices = pair_order.shape[0]
    device = jnp.arange(devices, dtype=jnp.int32)
    far_core, far_y = lax.rem(device % 2 + core, 2), lax.rem(device // 8 % 2 + y, 2)
    row = (far_core * 16 + far_y * 8 + device // 16) * sizes.tokens
    mirrored = 2 * devices - 1 - pair_order
    block = jnp.concatenate([pair_order, mirrored])
    row = jnp.concatenate([row, row + sizes.half])
    local = device // 2 % 4 == x
    local = jnp.concatenate([local, local])
    rank = jnp.sum((local[None, :] & (block[None, :] < block[:, None])).astype(jnp.int32), axis=1)
    place = jnp.arange(sizes.local, dtype=jnp.int32)
    chosen = local[None, :] & (rank[None, :] == place[:, None])
    address = jnp.sum(jnp.where(chosen, row[None, :], 0), axis=1)
    held = jnp.sum(jnp.where(chosen, block[None, :], 0), axis=1)
    docs = jnp.arange(sizes.docs, dtype=jnp.int32)
    ends = jnp.sum(jnp.where(docs[None, :] <= docs[:, None], doc_lengths[None, :], 0), axis=1)
    query = jnp.arange(sizes.queries, dtype=jnp.int32)
    owner = z * 16 + y * 8 + lax.rem(x + query // 2, 4) * 2 + core
    own = jnp.sum(jnp.where(owner[:, None] == device[None, :], pair_order[None, :], 0), axis=1)
    own = jnp.where(query % 2 == 0, own, 2 * devices - 1 - own)
    first = own * sizes.half
    start = jnp.max(jnp.where(ends[None, :] <= first[:, None], ends[None, :], 0), axis=1)
    low = jnp.sum((held[None, :] < (start // sizes.half)[:, None]).astype(jnp.int32), axis=1)
    high = jnp.sum((held[None, :] <= own[:, None]).astype(jnp.int32), axis=1)
    return jnp.concatenate([address, held, ends, own, low, high]).astype(jnp.int32)


def from_x(a, step):
    return lax.ppermute(a, "x", [((i + step) % 4, i) for i in range(4)])


def swap(a, axis):
    return lax.ppermute(a, axis, [(0, 1), (1, 0)])


def added(*terms):
    return sum(t.astype(jnp.float32) for t in terms).astype(jnp.bfloat16)


def over_z(a):
    return lax.all_to_all(a, "z", 0, 0, tiled=True)


def gathered_x(queries, grad_out):
    both = jnp.concatenate([queries, grad_out], axis=0)
    pieces = [both]
    for step in (1, 2, 3):
        pieces.append(from_x(both, step))
    return pieces


def gathered_keys(keys, values):
    kv = jnp.concatenate([keys, values], axis=1)
    near = over_z(jnp.tile(kv, (8, 1)))
    far = swap(near, "y")
    near_other = swap(near, "core")
    far_other = swap(far, "core")
    return [near, far, near_other, far_other]


def scattered_keys(own, other, tokens):
    n = 8 * tokens
    other = swap(other, "core")
    far = swap(added(own[n:], other[n:]), "y")
    column = over_z(added(own[:n], other[:n], far))
    column = column.reshape(8, tokens, -1).astype(jnp.float32)
    return jnp.sum(column, axis=0).astype(jnp.bfloat16)


def summed_x(first, second, tokens):
    totals = [a[:tokens].astype(jnp.float32) for a in (first, second)]
    for step in (1, 2, 3):
        at = slice((4 - step) * tokens, (5 - step) * tokens)
        arrived = from_x(jnp.concatenate([first[at], second[at]], axis=0), step)
        totals[0] = totals[0] + arrived[:tokens].astype(jnp.float32)
        totals[1] = totals[1] + arrived[tokens:].astype(jnp.float32)
    return totals


def shared_stats(stats):
    arrived = [stats]
    for step in (1, 2, 3):
        arrived.append(from_x(stats, step))
    return arrived


def grads_of(queries, keys, values, grad_out, pair_order, doc_lengths):
    tokens, hdim = keys.shape
    width = queries.shape[1]
    sizes = Sizes(tokens, width, hdim, pair_order.shape[0], doc_lengths.shape[0])
    spot = [lax.axis_index(a) for a in AXES]
    table = index_table(sizes, pair_order, doc_lengths, *spot)
    pieces = gathered_x(queries, grad_out) + gathered_keys(keys, values)
    pieces = [pltpu.with_memory_space_constraint(p, pltpu.HBM) for p in pieces]
    out_parts, stats = forward(sizes, table, pieces)
    stats = shared_stats(stats)
    dq_parts, *terms = backward(sizes, table, pieces, stats)
    total = sum(stats[i][(8 - 2 * i) % 8 : (8 - 2 * i) % 8 + 2, 0, :] for i in range(GROUP))
    total = total.reshape(2, sizes.heads, sizes.half)
    total = jnp.swapaxes(total, 1, 2).reshape(tokens, sizes.heads, 1)
    out, query_grad = summed_x(out_parts, dq_parts, tokens)
    out = out.reshape(tokens, sizes.heads, hdim) / total
    out = out.astype(jnp.bfloat16).reshape(tokens, width)
    grads = scattered_keys(*terms, tokens)
    return out, query_grad.astype(jnp.bfloat16), grads[:, :hdim], grads[:, hdim:]


def solution(mesh):
    torus = Mesh(mesh.devices.reshape(*DIMS, mesh.shape["dp"]), AXES + ("dp",))
    rows = P(DP_CTX, None)
    return jax.shard_map(
        grads_of,
        mesh=torus,
        in_specs=(rows, rows, rows, rows, P("dp"), P("dp")),
        out_specs=(rows, rows, rows, rows),
        check_vma=False,
    )
```
